256 devices in a mesh: cond: 2 (over z_hi), gx: 8 (over y, core), yz: 16 (over x, z_lo).
Axes of the slice: x: 4, y: 4, z: 8 (z_hi: 2, z_lo: 4; z = z_hi * 4 + z_lo), core: 2. Of those that a mesh axis runs over, the one named last changes fastest.
Arguments:
- adjoint: float32 [2, 5, 64, 256, 256], P('cond', None, 'gx', 'yz'), may hold values from -6 to 6
- objective_gradient: float32 [2, 5, 64, 256, 256], P('cond', None, 'gx', 'yz'), may hold values from -6 to 6
- diagonal: float32 [64, 256, 256], P('gx', 'yz'), may hold values from 4 to 12
- flux_blocks: float32 [2, 6, 5, 5], P('cond'), may hold values from -1 to 1
- flux_sensitivity: bfloat16 [2, 5, 64, 256, 256], P('cond', None, 'gx', 'yz'), may hold values from -6 to 6
- surface_mask: int32 [64, 256, 256], P('gx', 'yz'), may hold values 0 or 1
- patch_band_slot: int32 [64, 256], P('gx', 'yz'), may hold values from 0 to 62
- design_basis: float32 [256, 128], replicated, may hold values from -0.015625 to 0.015625
- condition_weights: int32 [2], replicated, may hold values from 1 to 999, as said below
Outputs:
- smoothed: float32 [2, 5, 64, 256, 256], P('cond', None, 'gx', 'yz')
- residual: float32 [2, 5, 64, 256, 256], P('cond', None, 'gx', 'yz')
- design_gradient: float32 [4096], P(('gx', 'yz'))
The draws below stay inside these ranges and needn't reach their ends.
Inputs may be any that keep to these rules, and one draw needn't show every extreme that they name: `condition_weights`: positive integer weights; one condition has weight 999.
All inputs are finite; a program needn't handle non-finite values. No bound on the sum of `surface_mask` on one device may be relied on, other than what follows from the above.
Results may differ from the reference program's by a relative error of at most 0.0003.
Values sent between devices are 32-bit elements; how exact they have to be, the bound alone decides.
No kernel may reach another device: no remote copies, remote signals or barrier semaphores. Data moves between devices by JAX's collectives and lax.ppermute only.
A program may use at most 64 MiB of HBM per device.

```python
import math
import jax
import jax.numpy as jnp
import numpy as np
from jax import lax

NZ = 256
NVAR = 5
BAND = 128
BAND_SLOTS = 63
COND = 2
CELLS_FIRST = 64
CELLS_SECOND = 256


def draw_condition_weights(key, part):
    drawn = jax.random.randint(jax.random.fold_in(key, 7), (COND,), 1, 1000, dtype=jnp.int32)
    chosen = jax.random.randint(jax.random.fold_in(key, 8), (), 0, COND, dtype=jnp.int32)
    return jnp.where(jnp.arange(COND, dtype=jnp.int32) == chosen, jnp.int32(999), drawn)


def touch_ends(array, own_key, least, top_value):
    longest = array.shape.index(max(array.shape))
    spots = []
    for shift in (0, 1):
        where = [jax.random.randint(jax.random.fold_in(own_key, axis), (), 0, length) for axis, length in enumerate(array.shape)]
        where[longest] = (where[longest] + shift) % array.shape[longest]
        spots.append(tuple(where))
    return array.at[spots[0]].set(least).at[spots[1]].set(top_value)


def level_of(stream_key, dims, cuts, low, high):
    level = 1.0
    for dim, blocks in cuts:
        steps = jax.random.uniform(jax.random.fold_in(jax.random.fold_in(stream_key, 6), dim), (blocks,), jnp.float32, low / len(cuts), high / len(cuts))
        level = level * jnp.repeat(jnp.exp(steps), dims[dim] // blocks).reshape((-1,) + (1,) * (len(dims) - 1 - dim))
    return level


def rank_table(count, skew):
    loads = [(1 << 20) // math.isqrt(grade ** skew) + 1 for grade in range(1, count + 1)]
    scale = 1 + sum(loads) // (1 << 30)
    return np.cumsum(np.array([max(1, weight // scale) for weight in loads]))


def ranked(own_key, extent, amount, lean):
    grid = rank_table(amount, lean)
    lot = jax.random.randint(jax.random.fold_in(own_key, 1), extent, 0, int(grid[amount - 1]))
    grade = jnp.searchsorted(jnp.asarray(grid, jnp.int32), lot, side="right")
    return jax.random.permutation(jax.random.fold_in(own_key, 2), amount)[grade].astype(jnp.int32)


def centred(key, shape, width, limit, pieces=(), kind=jnp.bfloat16):
    values = width * jax.random.normal(key, shape, jnp.float32)
    if pieces:
        values = values * level_of(key, shape, pieces, -0.22, 0.18)
    return jnp.clip(values, -limit, limit).astype(kind)


def setup_inputs(seed: int = 0) -> dict:
    streams_of = jax.random.split(jax.random.key(seed), 10)
    return {
        "adjoint": centred(streams_of[0], (COND, NVAR, CELLS_FIRST, CELLS_SECOND, NZ), 1.0, 6.0, ((0, 2), (2, 8), (3, 16)), jnp.float32),
        "objective_gradient": centred(streams_of[1], (COND, NVAR, CELLS_FIRST, CELLS_SECOND, NZ), 1.0, 6.0, ((0, 2), (2, 8), (3, 16)), jnp.float32),
        "diagonal": jnp.clip(jnp.exp(math.log(12.0) - 1.0986123 * jax.random.uniform(streams_of[2], (CELLS_FIRST, CELLS_SECOND, NZ), jnp.float32) ** level_of(streams_of[2], (CELLS_FIRST, CELLS_SECOND, NZ), ((0, 8), (1, 16)), -0.2, 0.2)), 4.0, 12.0),
        "flux_blocks": centred(streams_of[3], (COND, 6, NVAR, NVAR), (6 * NVAR) ** -0.5, 1.0, ((0, 2),), jnp.float32),
        "flux_sensitivity": centred(streams_of[4], (COND, NVAR, CELLS_FIRST, CELLS_SECOND, NZ), 1.0, 6.0, ((0, 2), (2, 8), (3, 16))),
        "surface_mask": touch_ends((jax.random.randint(streams_of[5], (CELLS_FIRST, CELLS_SECOND, NZ), 0, 4) < 1).astype(jnp.int32), jax.random.fold_in(streams_of[5], 1), 0, 1),
        "patch_band_slot": touch_ends(ranked(streams_of[6], (CELLS_FIRST, CELLS_SECOND), BAND_SLOTS, 2), jax.random.fold_in(streams_of[6], 3), 0, BAND_SLOTS - 1).astype(jnp.int32),
        "design_basis": centred(streams_of[7], (NZ, BAND), (NZ * CELLS_FIRST * CELLS_SECOND // 32) ** -0.5, 0.015625, (), jnp.float32),
        "condition_weights": draw_condition_weights(jax.random.fold_in(streams_of[9], 71), 0),
    }


relaxation = 0.8
neighbour_starts = ((2, 1, 1), (0, 1, 1), (1, 2, 1), (1, 0, 1), (1, 1, 2), (1, 1, 0))


def apply_operator(padded_field, diagonal, blocks):
    size_x = padded_field.shape[1] - 2
    size_y = padded_field.shape[2] - 2
    size_z = padded_field.shape[3] - 2
    result = diagonal * padded_field[:, 1:-1, 1:-1, 1:-1]
    for direction in range(6):
        start_x, start_y, start_z = neighbour_starts[direction]
        shifted = padded_field[:, start_x:start_x + size_x, start_y:start_y + size_y, start_z:start_z + size_z]
        result = result - jnp.einsum("ec,exyz->cxyz", blocks[direction], shifted, precision=lax.Precision.HIGHEST)
    return result


def spread_bands(slot_lookup):
    halfway = slot_lookup.shape[1] // 2
    first_half = jnp.pad(slot_lookup[:, :halfway], ((0, 1), (0, 0)))
    second_half = jnp.pad(slot_lookup[:, halfway:], ((1, 0), (0, 0)))
    return (first_half + second_half).reshape(-1)


def reference(adjoint, objective_gradient, diagonal, flux_blocks, flux_sensitivity, surface_mask, patch_band_slot, design_basis, condition_weights):
    def condition_solve(inputs):
        start_field, source, blocks, sensitivity = inputs

        def operate(values):
            return apply_operator(jnp.pad(values, ((0, 0), (1, 1), (1, 1), (1, 1))), diagonal, blocks)

        relaxed = start_field + (relaxation * (source - operate(start_field))) / diagonal
        smoothed = relaxed + (relaxation * (source - operate(relaxed))) / diagonal
        residual = source - operate(smoothed)
        surface = surface_mask.astype(jnp.float32) * jnp.sum(smoothed * sensitivity.astype(jnp.float32), axis=0)
        projected_gradient = jnp.dot(surface.reshape(-1, NZ), design_basis, precision=lax.Precision.HIGHEST, preferred_element_type=jnp.float32)
        slot_lookup = jax.ops.segment_sum(projected_gradient, patch_band_slot.reshape(-1), num_segments=BAND_SLOTS)
        return smoothed, residual, spread_bands(slot_lookup)

    smoothed, residual, gradients = lax.map(condition_solve, (adjoint, objective_gradient, flux_blocks, flux_sensitivity))
    weights_float = condition_weights.astype(jnp.float32)
    shares = weights_float / jnp.sum(weights_float)
    design_gradient = jnp.sum(shares[:, None] * gradients, axis=0)
    return smoothed, residual, design_gradient
```

```python
import functools

import jax
import jax.numpy as jnp
from jax import lax
from jax.experimental import pallas as pl
from jax.experimental.pallas import tpu as pltpu
from jax.sharding import Mesh
from jax.sharding import PartitionSpec as P

NDES = 4096
GX = ("gx_0", "gx_1")
YZ = ("yz_0", "yz_1")
RING = ("cond", "yz_1")
SPREAD = ("gx_0", "gx_1", "yz_0")
RELAXATION = 0.8
HIGHEST = lax.Precision.HIGHEST

VMEM = pl.BlockSpec(memory_space=pltpu.VMEM)
SMEM = pl.BlockSpec(memory_space=pltpu.SMEM)


def f32(*shape):
    return jax.ShapeDtypeStruct(shape, jnp.float32)


def position():
    gx = lax.axis_index("gx_0") * 2 + lax.axis_index("gx_1")
    yz = lax.axis_index("yz_0") * 4 + lax.axis_index("yz_1")
    return gx, yz


def write_sides(read, nvar, nx, ny, xa_ref, xb_ref, ya_ref, yb_ref):
    gx, yz = position()
    gx_even, yz_even = lax.rem(gx, 2) == 0, lax.rem(yz, 2) == 0
    for k in range(nvar):
        low, high = read(k, 0), read(k, nx - 1)
        xa_ref[k] = jnp.where(gx_even, high, low)
        xb_ref[k] = jnp.where(gx_even, low, high)
        for x in range(nx):
            slab = read(k, x)
            first, last = slab[0:1], slab[ny - 1 : ny]
            ya_ref[k, x : x + 1, :] = jnp.where(yz_even, last, first)
            yb_ref[k, x : x + 1, :] = jnp.where(yz_even, first, last)


def sides_kernel(v_ref, xa_ref, xb_ref, ya_ref, yb_ref):
    nvar, nx, ny, _ = v_ref.shape
    write_sides(lambda k, x: v_ref[k, x], nvar, nx, ny, xa_ref, xb_ref, ya_ref, yb_ref)


def neighbour_sums(v_ref, blocks_ref, x):
    nvar, nx, ny, nz = v_ref.shape
    row = lax.broadcasted_iota(jnp.int32, (ny, nz), 0)
    lane = lax.broadcasted_iota(jnp.int32, (ny, nz), 1)
    sums = [None] * nvar
    for e in range(nvar):
        centre = v_ref[e, x]
        shifted = {}
        if x + 1 < nx:
            shifted[0] = v_ref[e, x + 1]
        if x > 0:
            shifted[1] = v_ref[e, x - 1]
        shifted[2] = jnp.where(row == ny - 1, 0.0, pltpu.roll(centre, ny - 1, 0))
        shifted[3] = jnp.where(row == 0, 0.0, pltpu.roll(centre, 1, 0))
        shifted[4] = jnp.where(lane == nz - 1, 0.0, pltpu.roll(centre, nz - 1, 1))
        shifted[5] = jnp.where(lane == 0, 0.0, pltpu.roll(centre, 1, 1))
        for d, values in shifted.items():
            for k in range(nvar):
                term = blocks_ref[0, d, e, k] * values
                sums[k] = term if sums[k] is None else sums[k] + term
    return sums


def inner_sweep_kernel(blocks_ref, v_ref, source_ref, diagonal_ref, out_ref):
    nvar, nx, _, _ = v_ref.shape
    for x in range(nx):
        sums = neighbour_sums(v_ref, blocks_ref, x)
        diagonal = diagonal_ref[x]
        scale = RELAXATION / diagonal
        for k in range(nvar):
            value = v_ref[k, x]
            out_ref[k, x] = value + scale * (source_ref[k, x] - diagonal * value + sums[k])


def inner_residual_kernel(blocks_ref, v_ref, source_ref, diagonal_ref, out_ref):
    nvar, nx, _, _ = v_ref.shape
    for x in range(nx):
        sums = neighbour_sums(v_ref, blocks_ref, x)
        diagonal = diagonal_ref[x]
        for k in range(nvar):
            out_ref[k, x] = source_ref[k, x] - diagonal * v_ref[k, x] + sums[k]


def add_halo(blocks_ref, inner_ref, diagonal_ref, xa_ref, xb_ref, ya_ref, yb_ref, out_ref):
    nvar, nx, ny, nz = inner_ref.shape
    gx, yz = position()
    gx_even, yz_even = lax.rem(gx, 2) == 0, lax.rem(yz, 2) == 0
    has_low_x, has_high_x = gx > 0, gx < 7
    has_low_y, has_high_y = yz > 0, yz < 15

    def halo_sums(direction, pick):
        sums = [None] * nvar
        for e in range(nvar):
            values = pick(e)
            for k in range(nvar):
                term = blocks_ref[0, direction, e, k] * values
                sums[k] = term if sums[k] is None else sums[k] + term
        return sums

    def picker(even, a_ref, b_ref, exists):
        return lambda e: jnp.where(exists, jnp.where(even, a_ref[e], b_ref[e]), 0.0)

    high_y = halo_sums(2, picker(yz_even, ya_ref, yb_ref, has_high_y))
    low_y = halo_sums(3, picker(yz_even, yb_ref, ya_ref, has_low_y))
    row = lax.broadcasted_iota(jnp.int32, (8, nz), 0)
    for x in range(nx):
        if x == 0:
            at_x = halo_sums(1, picker(gx_even, xb_ref, xa_ref, has_low_x))
        elif x == nx - 1:
            at_x = halo_sums(0, picker(gx_even, xa_ref, xb_ref, has_high_x))
        else:
            at_x = None
        for start in range(0, ny, 8):
            rows = slice(start, start + 8)
            scale = None if diagonal_ref is None else RELAXATION / diagonal_ref[x, rows]
            for k in range(nvar):
                more = None
                if start == 0:
                    more = jnp.where(row == 0, low_y[k][x : x + 1], 0.0)
                if start == ny - 8:
                    last = jnp.where(row == 7, high_y[k][x : x + 1], 0.0)
                    more = last if more is None else more + last
                if at_x is not None:
                    more = at_x[k][rows] if more is None else more + at_x[k][rows]
                value = inner_ref[k, x, rows]
                if more is not None:
                    value = value + (more if scale is None else scale * more)
                out_ref[k, x, rows] = value


def outer_sweep_kernel(
    blocks_ref, inner_ref, diagonal_ref, xa_ref, xb_ref, ya_ref, yb_ref,
    out_ref, next_xa_ref, next_xb_ref, next_ya_ref, next_yb_ref,
):
    nvar, nx, ny, _ = inner_ref.shape
    add_halo(blocks_ref, inner_ref, diagonal_ref, xa_ref, xb_ref, ya_ref, yb_ref, out_ref)
    write_sides(
        lambda k, x: out_ref[k, x], nvar, nx, ny, next_xa_ref, next_xb_ref, next_ya_ref, next_yb_ref
    )


def last_sweep_kernel(
    blocks_ref, weights_ref, inner_ref, diagonal_ref, xa_ref, xb_ref, ya_ref, yb_ref,
    sensitivity_ref, mask_ref, slot_ref, basis_ref,
    out_ref, next_xa_ref, next_xb_ref, next_ya_ref, next_yb_ref, gradient_ref, surface_ref,
):
    outer_sweep_kernel(
        blocks_ref, inner_ref, diagonal_ref, xa_ref, xb_ref, ya_ref, yb_ref,
        out_ref, next_xa_ref, next_xb_ref, next_ya_ref, next_yb_ref,
    )
    nvar, nx, ny, _ = inner_ref.shape
    for x in range(nx):
        total = out_ref[0, x] * sensitivity_ref[0, x].astype(jnp.float32)
        for k in range(1, nvar):
            total = total + out_ref[k, x] * sensitivity_ref[k, x].astype(jnp.float32)
        surface_ref[x * ny : (x + 1) * ny, :] = mask_ref[x].astype(jnp.float32) * total
    projected = jnp.dot(
        surface_ref[...], basis_ref[...], precision=HIGHEST, preferred_element_type=jnp.float32
    )
    patches, band = projected.shape
    half = band // 2
    pairs = NDES // band
    wanted = lax.broadcasted_iota(jnp.int32, (2 * pairs, patches), 0)
    wanted = jnp.where(wanted < pairs, 2 * wanted, 2 * (wanted - pairs) + 1)
    onehot = (wanted == slot_ref[...]).astype(jnp.float32)
    by_slot = jnp.dot(onehot, projected, precision=HIGHEST, preferred_element_type=jnp.float32)
    even, odd = by_slot[:pairs], pltpu.roll(by_slot[pairs:], half, 1)
    row = lax.broadcasted_iota(jnp.int32, (pairs, band), 0)
    lane = lax.broadcasted_iota(jnp.int32, (pairs, band), 1)
    before = jnp.where(row == 0, 0.0, pltpu.roll(odd, 1, 0))
    gradient = even + jnp.where(lane < half, before, odd)
    mine = jnp.where(lax.axis_index("cond") == 0, weights_ref[0], weights_ref[1])
    total = weights_ref[0].astype(jnp.float32) + weights_ref[1].astype(jnp.float32)
    one = jnp.ones((pairs, band), jnp.float32)
    gradient_ref[...] = gradient * ((one * mine.astype(jnp.float32)) / (one * total))


def outer_residual_kernel(
    blocks_ref, inner_ref, xa_ref, xb_ref, ya_ref, yb_ref, out_ref,
):
    add_halo(blocks_ref, inner_ref, None, xa_ref, xb_ref, ya_ref, yb_ref, out_ref)


def swap_a(n):
    return [(i, i ^ 1) for i in range(n)]


def swap_b(n):
    return [(i, (((i + 1) ^ 1) - 1) % n) for i in range(n)]


def exchange(xa, xb, ya, yb):
    far = lax.ppermute(yb, YZ, swap_b(16))
    near = lax.ppermute(ya, YZ, swap_a(16))
    chip = lax.ppermute(xb, GX, swap_b(8))
    core = lax.ppermute(xa, GX, swap_a(8))
    return core, chip, near, far


def local(
    adjoint,
    objective_gradient,
    diagonal,
    flux_blocks,
    flux_sensitivity,
    surface_mask,
    patch_band_slot,
    design_basis,
    condition_weights,
):
    v, source, sensitivity = adjoint[0], objective_gradient[0], flux_sensitivity[0]
    nvar, nx, ny, nz = v.shape
    field = f32(nvar, nx, ny, nz)
    sides = (f32(nvar, ny, nz), f32(nvar, ny, nz), f32(nvar, nx, nz), f32(nvar, nx, nz))
    slot = patch_band_slot.reshape(1, -1)

    first = pl.pallas_call(
        sides_kernel, out_shape=sides, in_specs=[VMEM], out_specs=[VMEM] * 4, name="sides"
    )(v)
    halo = exchange(*first)
    inner_sweep = pl.pallas_call(
        inner_sweep_kernel, out_shape=field, in_specs=[SMEM] + [VMEM] * 3, out_specs=VMEM, name="inner_sweep"
    )
    inner = inner_sweep(flux_blocks, v, source, diagonal)
    relaxed, *second = pl.pallas_call(
        outer_sweep_kernel,
        out_shape=(field, *sides),
        in_specs=[SMEM] + [VMEM] * 6,
        out_specs=[VMEM] * 5,
        name="outer_sweep",
    )(flux_blocks, inner, diagonal, *halo)

    halo = exchange(*second)
    inner = inner_sweep(flux_blocks, relaxed, source, diagonal)
    smoothed, xa, xb, ya, yb, gradient = pl.pallas_call(
        last_sweep_kernel,
        out_shape=(field, *sides, f32(NDES // 128, 128)),
        in_specs=[SMEM, SMEM] + [VMEM] * 10,
        out_specs=[VMEM] * 6,
        scratch_shapes=[pltpu.VMEM((nx * ny, nz), jnp.float32)],
        name="last_sweep",
    )(flux_blocks, condition_weights, inner, diagonal, *halo, sensitivity, surface_mask, slot, design_basis)

    halo = exchange(xa, xb, ya, yb)
    parts = lax.all_to_all(gradient, SPREAD, 0, 0, tiled=True)
    total = jnp.sum(parts, axis=0, keepdims=True)
    total = total + lax.ppermute(total, RING, [(i, i ^ 1) for i in range(8)])
    total = total + lax.ppermute(total, RING, [(i, (((i + 1) ^ 1) - 1) % 8) for i in range(8)])
    total = total + lax.ppermute(total, RING, [(0, 3), (3, 0), (1, 6), (6, 1), (2, 5), (5, 2), (4, 7), (7, 4)])
    design_gradient = lax.dynamic_slice(total, (0, lax.axis_index("yz_1") * 32), (1, 32))[0]

    inner = pl.pallas_call(
        inner_residual_kernel, out_shape=field, in_specs=[SMEM] + [VMEM] * 3, out_specs=VMEM, name="inner_residual"
    )(flux_blocks, smoothed, source, diagonal)
    residual = pl.pallas_call(
        outer_residual_kernel, out_shape=field, in_specs=[SMEM] + [VMEM] * 5, out_specs=VMEM, name="outer_residual"
    )(flux_blocks, inner, *halo)
    return smoothed[None], residual[None], design_gradient


def solution(mesh):
    torus = Mesh(
        mesh.devices.reshape(mesh.shape["cond"], 4, 2, 4, 4),
        ("cond", "gx_0", "gx_1", "yz_0", "yz_1"),
    )
    in_specs = (
        P("cond", None, GX, YZ, None),
        P("cond", None, GX, YZ, None),
        P(GX, YZ, None),
        P("cond", None, None, None),
        P("cond", None, GX, YZ, None),
        P(GX, YZ, None),
        P(GX, YZ),
        P(),
        P(),
    )
    out_specs = (P("cond", None, GX, YZ, None), P("cond", None, GX, YZ, None), P(GX + YZ))
    return jax.shard_map(local, mesh=torus, in_specs=in_specs, out_specs=out_specs, check_vma=False)
```

```python
import jax
import jax.numpy as jnp
from jax import lax
from jax.experimental import pallas as pl
from jax.experimental.pallas import tpu as pltpu
from jax.sharding import Mesh
from jax.sharding import PartitionSpec as P


NDES = 4096
GX = ("gx_0", "gx_1")
YZ = ("yz_0", "yz_1")
RING = ("cond", "yz_1")
SPREAD = ("gx_0", "gx_1", "yz_0")
RELAXATION = 0.8
HIGHEST = lax.Precision.HIGHEST

VMEM = pl.BlockSpec(memory_space=pltpu.VMEM)
SMEM = pl.BlockSpec(memory_space=pltpu.SMEM)


def f32(*shape):
    return jax.ShapeDtypeStruct(shape, jnp.float32)


def kept(*shape):
    return pltpu.VMEM(shape, jnp.float32)


def near_core(x):
    return pltpu.with_memory_space_constraint(x, pltpu.VMEM)


def call(kernel, **options):
    params = pltpu.CompilerParams(vmem_limit_bytes=8 * 2**20)
    return pl.pallas_call(kernel, compiler_params=params, **options)


def position():
    gx = lax.axis_index("gx_0") * 2 + lax.axis_index("gx_1")
    yz = lax.axis_index("yz_0") * 4 + lax.axis_index("yz_1")
    return gx, yz


def write_sides(read, nvar, nx, ny, xa_ref, xb_ref, ya_ref, yb_ref):
    gx, yz = position()
    gx_even, yz_even = lax.rem(gx, 2) == 0, lax.rem(yz, 2) == 0
    for k in range(nvar):
        low, high = read(k, 0), read(k, nx - 1)
        xa_ref[k] = jnp.where(gx_even, high, low)
        xb_ref[k] = jnp.where(gx_even, low, high)
        for x in range(nx):
            slab = read(k, x)
            first, last = slab[0:1], slab[ny - 1 : ny]
            ya_ref[k, x : x + 1, :] = jnp.where(yz_even, last, first)
            yb_ref[k, x : x + 1, :] = jnp.where(yz_even, first, last)


def sides_kernel(v_ref, xa_ref, xb_ref, ya_ref, yb_ref):
    nvar, nx, ny, _ = v_ref.shape
    write_sides(lambda k, x: v_ref[k, x], nvar, nx, ny, xa_ref, xb_ref, ya_ref, yb_ref)


def neighbour_sums(v_ref, blocks_ref, x):
    nvar, nx, ny, nz = v_ref.shape
    row = lax.broadcasted_iota(jnp.int32, (ny, nz), 0)
    lane = lax.broadcasted_iota(jnp.int32, (ny, nz), 1)
    sums = [None] * nvar
    for e in range(nvar):
        centre = v_ref[e, x]
        shifted = {}
        if x + 1 < nx:
            shifted[0] = v_ref[e, x + 1]
        if x > 0:
            shifted[1] = v_ref[e, x - 1]
        shifted[2] = jnp.where(row == ny - 1, 0.0, pltpu.roll(centre, ny - 1, 0))
        shifted[3] = jnp.where(row == 0, 0.0, pltpu.roll(centre, 1, 0))
        shifted[4] = jnp.where(lane == nz - 1, 0.0, pltpu.roll(centre, nz - 1, 1))
        shifted[5] = jnp.where(lane == 0, 0.0, pltpu.roll(centre, 1, 1))
        for d, values in shifted.items():
            for k in range(nvar):
                term = blocks_ref[e, k, 0, d] * values
                sums[k] = term if sums[k] is None else sums[k] + term
    return sums


def inner_sweep_kernel(blocks_ref, v_ref, source_ref, diagonal_ref, out_ref):
    nvar, nx, _, _ = v_ref.shape
    for x in range(nx):
        sums = neighbour_sums(v_ref, blocks_ref, x)
        diagonal = diagonal_ref[x]
        scale = RELAXATION / diagonal
        for k in range(nvar):
            value = v_ref[k, x]
            out_ref[k, x] = value + scale * (source_ref[k, x] - diagonal * value + sums[k])


def inner_residual_kernel(blocks_ref, v_ref, source_ref, diagonal_ref, out_ref):
    nvar, nx, _, _ = v_ref.shape
    for x in range(nx):
        sums = neighbour_sums(v_ref, blocks_ref, x)
        diagonal = diagonal_ref[x]
        for k in range(nvar):
            out_ref[k, x] = source_ref[k, x] - diagonal * v_ref[k, x] + sums[k]


def add_halo(blocks_ref, inner_ref, diagonal_ref, xa_ref, xb_ref, ya_ref, yb_ref, out_ref):
    nvar, nx, ny, nz = inner_ref.shape
    gx, yz = position()
    gx_even, yz_even = lax.rem(gx, 2) == 0, lax.rem(yz, 2) == 0
    has_low_x, has_high_x = gx > 0, gx < 7
    has_low_y, has_high_y = yz > 0, yz < 15

    def halo_sums(direction, pick):
        sums = [None] * nvar
        for e in range(nvar):
            values = pick(e)
            for k in range(nvar):
                term = blocks_ref[e, k, 0, direction] * values
                sums[k] = term if sums[k] is None else sums[k] + term
        return sums

    def picker(even, a_ref, b_ref, exists):
        return lambda e: jnp.where(exists, jnp.where(even, a_ref[e], b_ref[e]), 0.0)

    high_y = halo_sums(2, picker(yz_even, ya_ref, yb_ref, has_high_y))
    low_y = halo_sums(3, picker(yz_even, yb_ref, ya_ref, has_low_y))
    row = lax.broadcasted_iota(jnp.int32, (8, nz), 0)
    for x in range(nx):
        if x == 0:
            at_x = halo_sums(1, picker(gx_even, xb_ref, xa_ref, has_low_x))
        elif x == nx - 1:
            at_x = halo_sums(0, picker(gx_even, xa_ref, xb_ref, has_high_x))
        else:
            at_x = None
        for start in range(0, ny, 8):
            rows = slice(start, start + 8)
            scale = None if diagonal_ref is None else RELAXATION / diagonal_ref[x, rows]
            for k in range(nvar):
                more = None
                if start == 0:
                    more = jnp.where(row == 0, low_y[k][x : x + 1], 0.0)
                if start == ny - 8:
                    last = jnp.where(row == 7, high_y[k][x : x + 1], 0.0)
                    more = last if more is None else more + last
                if at_x is not None:
                    more = at_x[k][rows] if more is None else more + at_x[k][rows]
                value = inner_ref[k, x, rows]
                if more is not None:
                    value = value + (more if scale is None else scale * more)
                out_ref[k, x, rows] = value


def outer_sweep_kernel(
    blocks_ref, inner_ref, diagonal_ref, xa_ref, xb_ref, ya_ref, yb_ref,
    out_ref, next_xa_ref, next_xb_ref, next_ya_ref, next_yb_ref,
):
    nvar, nx, ny, _ = inner_ref.shape
    add_halo(blocks_ref, inner_ref, diagonal_ref, xa_ref, xb_ref, ya_ref, yb_ref, out_ref)
    write_sides(
        lambda k, x: out_ref[k, x], nvar, nx, ny, next_xa_ref, next_xb_ref, next_ya_ref, next_yb_ref
    )


def last_sweep_kernel(
    blocks_ref, weights_ref, inner_ref, diagonal_ref, xa_ref, xb_ref, ya_ref, yb_ref,
    sensitivity_ref, mask_ref, slot_ref, basis_ref,
    out_ref, next_xa_ref, next_xb_ref, next_ya_ref, next_yb_ref, gradient_ref, surface_ref,
):
    outer_sweep_kernel(
        blocks_ref, inner_ref, diagonal_ref, xa_ref, xb_ref, ya_ref, yb_ref,
        out_ref, next_xa_ref, next_xb_ref, next_ya_ref, next_yb_ref,
    )
    nvar, nx, ny, _ = inner_ref.shape
    for x in range(nx):
        total = out_ref[0, x] * sensitivity_ref[0, x].astype(jnp.float32)
        for k in range(1, nvar):
            total = total + out_ref[k, x] * sensitivity_ref[k, x].astype(jnp.float32)
        surface_ref[x * ny : (x + 1) * ny, :] = mask_ref[x].astype(jnp.float32) * total
    projected = jnp.dot(
        surface_ref[...], basis_ref[...], precision=HIGHEST, preferred_element_type=jnp.float32
    )
    patches, band = projected.shape
    half = band // 2
    pairs = NDES // band
    wanted = lax.broadcasted_iota(jnp.int32, (2 * pairs, patches), 0)
    wanted = jnp.where(wanted < pairs, 2 * wanted, 2 * (wanted - pairs) + 1)
    lane = lax.broadcasted_iota(jnp.int32, (ny, patches), 1)
    repeat = lax.rem(lane, ny) == lax.broadcasted_iota(jnp.int32, (ny, patches), 0)
    slots = jnp.dot(
        slot_ref[...].astype(jnp.float32), repeat.astype(jnp.float32), preferred_element_type=jnp.float32
    )
    lane = lax.broadcasted_iota(jnp.int32, (nx, patches), 1)
    own = lax.div(lane, ny) == lax.broadcasted_iota(jnp.int32, (nx, patches), 0)
    slots = jnp.sum(jnp.where(own, slots, 0.0), axis=0, keepdims=True)
    onehot = (wanted.astype(jnp.float32) == slots).astype(jnp.float32)
    by_slot = jnp.dot(onehot, projected, precision=HIGHEST, preferred_element_type=jnp.float32)
    even, odd = by_slot[:pairs], pltpu.roll(by_slot[pairs:], half, 1)
    row = lax.broadcasted_iota(jnp.int32, (pairs, band), 0)
    lane = lax.broadcasted_iota(jnp.int32, (pairs, band), 1)
    before = jnp.where(row == 0, 0.0, pltpu.roll(odd, 1, 0))
    gradient = even + jnp.where(lane < half, before, odd)
    mine = jnp.where(lax.axis_index("cond") == 0, weights_ref[0], weights_ref[1])
    total = weights_ref[0].astype(jnp.float32) + weights_ref[1].astype(jnp.float32)
    one = jnp.ones((pairs, band), jnp.float32)
    gradient_ref[...] = gradient * ((one * mine.astype(jnp.float32)) / (one * total))


def outer_residual_kernel(
    blocks_ref, inner_ref, xa_ref, xb_ref, ya_ref, yb_ref, out_ref,
):
    add_halo(blocks_ref, inner_ref, None, xa_ref, xb_ref, ya_ref, yb_ref, out_ref)


def swap_a(n):
    return [(i, i ^ 1) for i in range(n)]


def swap_b(n):
    return [(i, (((i + 1) ^ 1) - 1) % n) for i in range(n)]


def exchange(xa, xb, ya, yb):
    far = lax.ppermute(yb, YZ, swap_b(16))
    near = lax.ppermute(ya, YZ, swap_a(16))
    chip = lax.ppermute(xb, GX, swap_b(8))
    core = lax.ppermute(xa, GX, swap_a(8))
    return tuple(near_core(x) for x in (core, chip, near, far))


def step(
    adjoint,
    objective_gradient,
    diagonal,
    flux_blocks,
    flux_sensitivity,
    surface_mask,
    patch_band_slot,
    design_basis,
    condition_weights,
):
    v, source = near_core(adjoint[0]), near_core(objective_gradient[0])
    sensitivity, mask = near_core(flux_sensitivity[0]), near_core(surface_mask)
    diagonal, basis = near_core(diagonal), near_core(design_basis)
    blocks = flux_blocks.transpose(2, 3, 0, 1)
    nvar, nx, ny, nz = v.shape
    field = kept(nvar, nx, ny, nz)
    sides = (kept(nvar, ny, nz), kept(nvar, ny, nz), kept(nvar, nx, nz), kept(nvar, nx, nz))

    first = call(
        sides_kernel, out_shape=sides, in_specs=[VMEM], out_specs=[VMEM] * 4, name="sides"
    )(v)
    halo = exchange(*first)
    inner_sweep = call(
        inner_sweep_kernel, out_shape=field, in_specs=[SMEM] + [VMEM] * 3, out_specs=VMEM, name="inner_sweep"
    )
    inner = inner_sweep(blocks, v, source, diagonal)
    relaxed, *second = call(
        outer_sweep_kernel,
        out_shape=(field, *sides),
        in_specs=[SMEM] + [VMEM] * 6,
        out_specs=[VMEM] * 5,
        name="outer_sweep",
    )(blocks, near_core(inner), diagonal, *halo)

    halo = exchange(*second)
    inner = inner_sweep(blocks, near_core(relaxed), source, diagonal)
    smoothed, xa, xb, ya, yb, gradient = call(
        last_sweep_kernel,
        out_shape=(field, *sides, kept(NDES // 128, 128)),
        in_specs=[SMEM, SMEM] + [VMEM] * 10,
        out_specs=[VMEM] * 6,
        scratch_shapes=[pltpu.VMEM((nx * ny, nz), jnp.float32)],
        name="last_sweep",
    )(blocks, condition_weights, near_core(inner), diagonal, *halo, sensitivity, mask, near_core(patch_band_slot), basis)

    parts = lax.all_to_all(gradient, SPREAD, 0, 0, tiled=True)
    total = jnp.sum(parts, axis=0, keepdims=True)
    total = total + lax.ppermute(total, RING, [(i, i ^ 1) for i in range(8)])
    halo = exchange(xa, xb, ya, yb)
    total = total + lax.ppermute(total, RING, [(i, (((i + 1) ^ 1) - 1) % 8) for i in range(8)])
    across = [(0, 3), (3, 0), (1, 6), (6, 1), (2, 5), (5, 2), (4, 7), (7, 4)]
    total = total + lax.ppermute(total, RING, across)
    design_gradient = lax.dynamic_slice(total, (0, lax.axis_index("yz_1") * 32), (1, 32))[0]

    inner = call(
        inner_residual_kernel,
        out_shape=field,
        in_specs=[SMEM] + [VMEM] * 3,
        out_specs=VMEM,
        name="inner_residual",
    )(blocks, near_core(smoothed), source, diagonal)
    residual = call(
        outer_residual_kernel,
        out_shape=f32(nvar, nx, ny, nz),
        in_specs=[SMEM] + [VMEM] * 5,
        out_specs=VMEM,
        name="outer_residual",
    )(blocks, near_core(inner), *halo)
    return smoothed[None], residual[None], design_gradient


def solution(mesh):
    torus = Mesh(
        mesh.devices.reshape(mesh.shape["cond"], 4, 2, 4, 4),
        ("cond", "gx_0", "gx_1", "yz_0", "yz_1"),
    )
    in_specs = (
        P("cond", None, GX, YZ, None),
        P("cond", None, GX, YZ, None),
        P(GX, YZ, None),
        P("cond", None, None, None),
        P("cond", None, GX, YZ, None),
        P(GX, YZ, None),
        P(GX, YZ),
        P(),
        P(),
    )
    out_specs = (P("cond", None, GX, YZ, None), P("cond", None, GX, YZ, None), P(GX + YZ))
    return jax.shard_map(step, mesh=torus, in_specs=in_specs, out_specs=out_specs, check_vma=False)
```

```python
import jax
import jax.numpy as jnp
from jax import lax
from jax.experimental import pallas as pl
from jax.experimental.pallas import tpu as pltpu
from jax.sharding import Mesh
from jax.sharding import PartitionSpec as P


NDES = 4096
GX = ("gx_0", "gx_1")
YZ = ("yz_0", "yz_1")
RING = ("cond", "yz_1")
SPREAD = ("gx_0", "gx_1", "yz_0")
RELAXATION = 0.8
HIGHEST = lax.Precision.HIGHEST

VMEM = pl.BlockSpec(memory_space=pltpu.VMEM)
HBM = pl.BlockSpec(memory_space=pltpu.HBM)
SMEM = pl.BlockSpec(memory_space=pltpu.SMEM)


def f32(*shape):
    return jax.ShapeDtypeStruct(shape, jnp.float32)


def kept(*shape):
    return pltpu.VMEM(shape, jnp.float32)


def far_from_core(x):
    return pltpu.with_memory_space_constraint(x, pltpu.HBM)


def near_core(x):
    return pltpu.with_memory_space_constraint(x, pltpu.VMEM)


def call(kernel, **options):
    params = pltpu.CompilerParams(vmem_limit_bytes=8 * 2**20)
    return pl.pallas_call(kernel, compiler_params=params, **options)


def position():
    gx = lax.axis_index("gx_0") * 2 + lax.axis_index("gx_1")
    yz = lax.axis_index("yz_0") * 4 + lax.axis_index("yz_1")
    return gx, yz


def write_sides(read, nvar, nx, ny, xa_ref, xb_ref, ya_ref, yb_ref):
    gx, yz = position()
    gx_even, yz_even = lax.rem(gx, 2) == 0, lax.rem(yz, 2) == 0
    for k in range(nvar):
        low, high = read(k, 0), read(k, nx - 1)
        xa_ref[k] = jnp.where(gx_even, high, low)
        xb_ref[k] = jnp.where(gx_even, low, high)
        for x in range(nx):
            slab = read(k, x)
            first, last = slab[0:1], slab[ny - 1 : ny]
            ya_ref[k, x : x + 1, :] = jnp.where(yz_even, last, first)
            yb_ref[k, x : x + 1, :] = jnp.where(yz_even, first, last)


def coefficient(table_ref, d, e, k, nvar, shape):
    tile = table_ref[pl.ds((d * nvar + e) * nvar + k, 8, stride=0), :]
    rows = jnp.concatenate([tile] * (shape[0] // 8), axis=0)
    return jnp.concatenate([rows] * (shape[1] // 128), axis=1)


def first_sides_kernel(v_hbm, v_ref, xa_ref, xb_ref, ya_ref, yb_ref, sem):
    copy = pltpu.make_async_copy(v_hbm, v_ref, sem)
    copy.start()
    copy.wait()
    nvar, nx, ny, _ = v_ref.shape
    write_sides(lambda k, x: v_ref[k, x], nvar, nx, ny, xa_ref, xb_ref, ya_ref, yb_ref)


def load_kernel(
    blocks_hbm, weights_hbm, source_hbm, diagonal_hbm, source_ref, diagonal_ref, table_ref,
    blocks_ref, weights_ref, sems,
):
    pairs = (
        (blocks_hbm, blocks_ref),
        (weights_hbm, weights_ref),
        (source_hbm, source_ref),
        (diagonal_hbm, diagonal_ref),
    )
    copies = [pltpu.make_async_copy(a, b, sems.at[i]) for i, (a, b) in enumerate(pairs)]
    for copy in copies:
        copy.start()
    nvar = source_ref.shape[0]
    for copy in copies[:2]:
        copy.wait()
    for d in range(6):
        for e in range(nvar):
            for k in range(nvar):
                row = (d * nvar + e) * nvar + k
                table_ref[row : row + 1, :] = jnp.full((1, 128), blocks_ref[e, k, 0, d])
    mine = jnp.where(lax.axis_index("cond") == 0, weights_ref[0], weights_ref[1])
    total = weights_ref[0].astype(jnp.float32) + weights_ref[1].astype(jnp.float32)
    one = jnp.ones((1, 128), jnp.float32)
    last = 6 * nvar * nvar
    table_ref[last : last + 1, :] = (one * mine.astype(jnp.float32)) / (one * total)
    for copy in copies[2:]:
        copy.wait()


def neighbour_sums(v_ref, blocks_ref, x):
    nvar, nx, ny, nz = v_ref.shape
    row = lax.broadcasted_iota(jnp.int32, (ny, nz), 0)
    lane = lax.broadcasted_iota(jnp.int32, (ny, nz), 1)
    sums = [None] * nvar
    for e in range(nvar):
        centre = v_ref[e, x]
        shifted = {}
        if x + 1 < nx:
            shifted[0] = v_ref[e, x + 1]
        if x > 0:
            shifted[1] = v_ref[e, x - 1]
        shifted[2] = jnp.where(row == ny - 1, 0.0, pltpu.roll(centre, ny - 1, 0))
        shifted[3] = jnp.where(row == 0, 0.0, pltpu.roll(centre, 1, 0))
        shifted[4] = jnp.where(lane == nz - 1, 0.0, pltpu.roll(centre, nz - 1, 1))
        shifted[5] = jnp.where(lane == 0, 0.0, pltpu.roll(centre, 1, 1))
        for d, values in shifted.items():
            for k in range(nvar):
                term = coefficient(blocks_ref, d, e, k, nvar, values.shape) * values
                sums[k] = term if sums[k] is None else sums[k] + term
    return sums


def inner_sweep_kernel(blocks_ref, v_ref, source_ref, diagonal_ref, out_ref):
    nvar, nx, _, _ = v_ref.shape
    for x in range(nx):
        sums = neighbour_sums(v_ref, blocks_ref, x)
        diagonal = diagonal_ref[x]
        scale = RELAXATION / diagonal
        for k in range(nvar):
            value = v_ref[k, x]
            out_ref[k, x] = value + scale * (source_ref[k, x] - diagonal * value + sums[k])


def inner_residual_kernel(blocks_ref, v_ref, source_ref, diagonal_ref, out_ref, v_hbm, sem):
    copy = pltpu.make_async_copy(v_ref, v_hbm, sem)
    copy.start()
    nvar, nx, _, _ = v_ref.shape
    for x in range(nx):
        sums = neighbour_sums(v_ref, blocks_ref, x)
        diagonal = diagonal_ref[x]
        for k in range(nvar):
            out_ref[k, x] = source_ref[k, x] - diagonal * v_ref[k, x] + sums[k]
    copy.wait()


def add_halo(blocks_ref, inner_ref, diagonal_ref, xa_ref, xb_ref, ya_ref, yb_ref, out_ref):
    nvar, nx, ny, nz = inner_ref.shape
    gx, yz = position()
    gx_even, yz_even = lax.rem(gx, 2) == 0, lax.rem(yz, 2) == 0
    has_low_x, has_high_x = gx > 0, gx < 7
    has_low_y, has_high_y = yz > 0, yz < 15

    def halo_sums(direction, pick):
        sums = [None] * nvar
        for e in range(nvar):
            values = pick(e)
            for k in range(nvar):
                term = coefficient(blocks_ref, direction, e, k, nvar, values.shape) * values
                sums[k] = term if sums[k] is None else sums[k] + term
        return sums

    def picker(even, a_ref, b_ref, exists):
        return lambda e: jnp.where(exists, jnp.where(even, a_ref[e], b_ref[e]), 0.0)

    high_y = halo_sums(2, picker(yz_even, ya_ref, yb_ref, has_high_y))
    low_y = halo_sums(3, picker(yz_even, yb_ref, ya_ref, has_low_y))
    row = lax.broadcasted_iota(jnp.int32, (8, nz), 0)
    for x in range(nx):
        if x == 0:
            at_x = halo_sums(1, picker(gx_even, xb_ref, xa_ref, has_low_x))
        elif x == nx - 1:
            at_x = halo_sums(0, picker(gx_even, xa_ref, xb_ref, has_high_x))
        else:
            at_x = None
        for start in range(0, ny, 8):
            rows = slice(start, start + 8)
            scale = None if diagonal_ref is None else RELAXATION / diagonal_ref[x, rows]
            for k in range(nvar):
                more = None
                if start == 0:
                    more = jnp.where(row == 0, low_y[k][x : x + 1], 0.0)
                if start == ny - 8:
                    last = jnp.where(row == 7, high_y[k][x : x + 1], 0.0)
                    more = last if more is None else more + last
                if at_x is not None:
                    more = at_x[k][rows] if more is None else more + at_x[k][rows]
                value = inner_ref[k, x, rows]
                if more is not None:
                    value = value + (more if scale is None else scale * more)
                out_ref[k, x, rows] = value


def outer_sweep_kernel(
    blocks_ref, inner_ref, diagonal_ref, xa_ref, xb_ref, ya_ref, yb_ref,
    out_ref, next_xa_ref, next_xb_ref, next_ya_ref, next_yb_ref,
):
    nvar, nx, ny, _ = inner_ref.shape
    add_halo(blocks_ref, inner_ref, diagonal_ref, xa_ref, xb_ref, ya_ref, yb_ref, out_ref)
    write_sides(
        lambda k, x: out_ref[k, x], nvar, nx, ny, next_xa_ref, next_xb_ref, next_ya_ref, next_yb_ref
    )


def last_sweep_kernel(
    blocks_ref, inner_ref, diagonal_ref, xa_ref, xb_ref, ya_ref, yb_ref,
    sensitivity_ref, mask_ref, slot_ref, basis_ref,
    out_ref, next_xa_ref, next_xb_ref, next_ya_ref, next_yb_ref, gradient_ref, surface_ref,
):
    outer_sweep_kernel(
        blocks_ref, inner_ref, diagonal_ref, xa_ref, xb_ref, ya_ref, yb_ref,
        out_ref, next_xa_ref, next_xb_ref, next_ya_ref, next_yb_ref,
    )
    nvar, nx, ny, _ = inner_ref.shape
    for x in range(nx):
        total = out_ref[0, x] * sensitivity_ref[0, x].astype(jnp.float32)
        for k in range(1, nvar):
            total = total + out_ref[k, x] * sensitivity_ref[k, x].astype(jnp.float32)
        surface_ref[x * ny : (x + 1) * ny, :] = mask_ref[x].astype(jnp.float32) * total
    projected = jnp.dot(
        surface_ref[...], basis_ref[...], precision=HIGHEST, preferred_element_type=jnp.float32
    )
    patches, band = projected.shape
    half = band // 2
    pairs = NDES // band
    wanted = lax.broadcasted_iota(jnp.int32, (2 * pairs, patches), 0)
    wanted = jnp.where(wanted < pairs, 2 * wanted, 2 * (wanted - pairs) + 1)
    lane = lax.broadcasted_iota(jnp.int32, (ny, patches), 1)
    repeat = lax.rem(lane, ny) == lax.broadcasted_iota(jnp.int32, (ny, patches), 0)
    slots = jnp.dot(
        slot_ref[...].astype(jnp.float32), repeat.astype(jnp.float32), preferred_element_type=jnp.float32
    )
    lane = lax.broadcasted_iota(jnp.int32, (nx, patches), 1)
    own = lax.div(lane, ny) == lax.broadcasted_iota(jnp.int32, (nx, patches), 0)
    slots = jnp.sum(jnp.where(own, slots, 0.0), axis=0, keepdims=True)
    onehot = (wanted.astype(jnp.float32) == slots).astype(jnp.float32)
    by_slot = jnp.dot(onehot, projected, precision=HIGHEST, preferred_element_type=jnp.float32)
    even, odd = by_slot[:pairs], pltpu.roll(by_slot[pairs:], half, 1)
    row = lax.broadcasted_iota(jnp.int32, (pairs, band), 0)
    lane = lax.broadcasted_iota(jnp.int32, (pairs, band), 1)
    before = jnp.where(row == 0, 0.0, pltpu.roll(odd, 1, 0))
    gradient = even + jnp.where(lane < half, before, odd)
    share = blocks_ref[pl.ds(6 * nvar * nvar, 8, stride=0), :]
    gradient_ref[...] = gradient * jnp.concatenate([share] * (pairs // 8), axis=0)


def outer_residual_kernel(
    blocks_ref, inner_ref, xa_ref, xb_ref, ya_ref, yb_ref, part_ref, other_ref, out_ref, piece_ref,
):
    add_halo(blocks_ref, inner_ref, None, xa_ref, xb_ref, ya_ref, yb_ref, out_ref)
    size = piece_ref.shape[1]
    total = part_ref[...] + other_ref[...]
    which = lax.axis_index("yz_1")
    piece = total[:, :size]
    for i in range(1, total.shape[1] // size):
        piece = jnp.where(which == i, total[:, i * size : (i + 1) * size], piece)
    piece_ref[...] = piece


def swap_a(n):
    return [(i, i ^ 1) for i in range(n)]


def swap_b(n):
    return [(i, (((i + 1) ^ 1) - 1) % n) for i in range(n)]


def exchange(xa, xb, ya, yb):
    far = lax.ppermute(yb, YZ, swap_b(16))
    near = lax.ppermute(ya, YZ, swap_a(16))
    chip = lax.ppermute(xb, GX, swap_b(8))
    core = lax.ppermute(xa, GX, swap_a(8))
    return tuple(near_core(x) for x in (core, chip, near, far))


def step(
    adjoint,
    objective_gradient,
    diagonal,
    flux_blocks,
    flux_sensitivity,
    surface_mask,
    patch_band_slot,
    design_basis,
    condition_weights,
):
    sensitivity, mask = near_core(flux_sensitivity[0]), near_core(surface_mask)
    basis = near_core(design_basis)
    _, nvar, nx, ny, nz = adjoint.shape
    field = kept(nvar, nx, ny, nz)
    sides = (kept(nvar, ny, nz), kept(nvar, ny, nz), kept(nvar, nx, nz), kept(nvar, nx, nz))

    v, *first = call(
        first_sides_kernel,
        out_shape=(field, *sides),
        in_specs=[HBM],
        out_specs=[VMEM] * 5,
        scratch_shapes=[pltpu.SemaphoreType.DMA],
        name="first_sides",
    )(far_from_core(adjoint[0]))
    v = near_core(v)
    halo = exchange(*first)
    arrays = (flux_blocks.transpose(2, 3, 0, 1), condition_weights, objective_gradient[0], diagonal)
    source, diagonal, table = call(
        load_kernel,
        out_shape=(field, kept(nx, ny, nz), kept(6 * nvar * nvar + 1, 128)),
        in_specs=[HBM] * 4,
        out_specs=[VMEM] * 3,
        scratch_shapes=[
            pltpu.SMEM((nvar, nvar, 1, 6), jnp.float32),
            pltpu.SMEM(condition_weights.shape, jnp.int32),
            pltpu.SemaphoreType.DMA((4,)),
        ],
        name="load",
    )(*(far_from_core(x) for x in arrays))
    source, diagonal, blocks = near_core(source), near_core(diagonal), near_core(table)
    inner_sweep = call(
        inner_sweep_kernel, out_shape=field, in_specs=[VMEM] * 4, out_specs=VMEM, name="inner_sweep"
    )
    inner = inner_sweep(blocks, v, source, diagonal)
    relaxed, *second = call(
        outer_sweep_kernel,
        out_shape=(field, *sides),
        in_specs=[VMEM] * 7,
        out_specs=[VMEM] * 5,
        name="outer_sweep",
    )(blocks, near_core(inner), diagonal, *halo)

    halo = exchange(*second)
    inner = inner_sweep(blocks, near_core(relaxed), source, diagonal)
    smoothed, xa, xb, ya, yb, gradient = call(
        last_sweep_kernel,
        out_shape=(field, *sides, kept(NDES // 128, 128)),
        in_specs=[VMEM] * 11,
        out_specs=[VMEM] * 6,
        scratch_shapes=[pltpu.VMEM((nx * ny, nz), jnp.float32)],
        name="last_sweep",
    )(blocks, near_core(inner), diagonal, *halo, sensitivity, mask, near_core(patch_band_slot), basis)

    parts = lax.all_to_all(gradient, SPREAD, 0, 0, tiled=True)
    total = jnp.sum(parts, axis=0, keepdims=True)
    total = total + lax.ppermute(total, RING, [(i, i ^ 1) for i in range(8)])
    halo = exchange(xa, xb, ya, yb)
    total = total + lax.ppermute(total, RING, [(i, (((i + 1) ^ 1) - 1) % 8) for i in range(8)])
    across = [(0, 3), (3, 0), (1, 6), (6, 1), (2, 5), (5, 2), (4, 7), (7, 4)]
    other = lax.ppermute(total, RING, across)

    inner, smoothed = call(
        inner_residual_kernel,
        out_shape=(field, pltpu.HBM((nvar, nx, ny, nz), jnp.float32)),
        in_specs=[VMEM] * 4,
        out_specs=[VMEM, HBM],
        scratch_shapes=[pltpu.SemaphoreType.DMA],
        name="inner_residual",
    )(blocks, near_core(smoothed), source, diagonal)
    residual, design_gradient = call(
        outer_residual_kernel,
        out_shape=(f32(nvar, nx, ny, nz), f32(1, 32)),
        in_specs=[VMEM] * 8,
        out_specs=[VMEM] * 2,
        name="outer_residual",
    )(blocks, near_core(inner), *halo, near_core(total), near_core(other))
    return smoothed[None], residual[None], design_gradient.reshape(-1)


def solution(mesh):
    torus = Mesh(
        mesh.devices.reshape(mesh.shape["cond"], 4, 2, 4, 4),
        ("cond", "gx_0", "gx_1", "yz_0", "yz_1"),
    )
    in_specs = (
        P("cond", None, GX, YZ, None),
        P("cond", None, GX, YZ, None),
        P(GX, YZ, None),
        P("cond", None, None, None),
        P("cond", None, GX, YZ, None),
        P(GX, YZ, None),
        P(GX, YZ),
        P(),
        P(),
    )
    out_specs = (P("cond", None, GX, YZ, None), P("cond", None, GX, YZ, None), P(GX + YZ))
    return jax.shard_map(step, mesh=torus, in_specs=in_specs, out_specs=out_specs, check_vma=False)
```

```python
import jax
import jax.numpy as jnp
from jax import lax
from jax.experimental import pallas as pl
from jax.experimental.pallas import tpu as pltpu
from jax.sharding import Mesh
from jax.sharding import PartitionSpec as P


NDES = 4096
GX = ("gx_0", "gx_1")
YZ = ("yz_0", "yz_1")
RING = ("cond", "yz_1")
SPREAD = ("gx_0", "gx_1", "yz_0")
RELAXATION = 0.8
HIGHEST = lax.Precision.HIGHEST

VMEM = pl.BlockSpec(memory_space=pltpu.VMEM)
HBM = pl.BlockSpec(memory_space=pltpu.HBM)
SMEM = pl.BlockSpec(memory_space=pltpu.SMEM)


def f32(*shape):
    return jax.ShapeDtypeStruct(shape, jnp.float32)


def kept(*shape):
    return pltpu.VMEM(shape, jnp.float32)


def far_from_core(x):
    return pltpu.with_memory_space_constraint(x, pltpu.HBM)


def near_core(x):
    return pltpu.with_memory_space_constraint(x, pltpu.VMEM)


def call(kernel, **options):
    params = pltpu.CompilerParams(vmem_limit_bytes=8 * 2**20)
    return pl.pallas_call(kernel, compiler_params=params, **options)


def position():
    gx = lax.axis_index("gx_0") * 2 + lax.axis_index("gx_1")
    yz = lax.axis_index("yz_0") * 4 + lax.axis_index("yz_1")
    return gx, yz


def write_sides(read, nvar, nx, ny, xa_ref, xb_ref, ya_ref, yb_ref):
    gx, yz = position()
    gx_even, yz_even = lax.rem(gx, 2) == 0, lax.rem(yz, 2) == 0
    for k in range(nvar):
        low, high = read(k, 0), read(k, nx - 1)
        xa_ref[k] = jnp.where(gx_even, high, low)
        xb_ref[k] = jnp.where(gx_even, low, high)
        for x in range(nx):
            slab = read(k, x)
            first, last = slab[0:1], slab[ny - 1 : ny]
            ya_ref[k, x : x + 1, :] = jnp.where(yz_even, last, first)
            yb_ref[k, x : x + 1, :] = jnp.where(yz_even, first, last)


def coefficient(table_ref, d, e, k, nvar, shape):
    tile = table_ref[pl.ds((d * nvar + e) * nvar + k, 8, stride=0), :]
    rows = jnp.concatenate([tile] * (shape[0] // 8), axis=0)
    return jnp.concatenate([rows] * (shape[1] // 128), axis=1)


def load_kernel(
    blocks_hbm, weights_hbm, v_hbm, source_hbm, diagonal_hbm,
    v_ref, source_ref, diagonal_ref, table_ref, xa_ref, xb_ref, ya_ref, yb_ref,
    blocks_ref, weights_ref, next_ref, wanted_ref, sems,
):
    pairs = (
        (blocks_hbm, blocks_ref),
        (weights_hbm, weights_ref),
        (v_hbm, v_ref),
        (source_hbm, source_ref),
        (diagonal_hbm, diagonal_ref),
    )
    copies = [pltpu.make_async_copy(a, b, sems.at[i]) for i, (a, b) in enumerate(pairs)]
    for copy in copies:
        copy.start()
    nvar, nx, ny, nz = v_ref.shape
    for copy in copies[:2]:
        copy.wait()
    for d in range(6):
        for e in range(nvar):
            for k in range(nvar):
                row = (d * nvar + e) * nvar + k
                table_ref[row : row + 1, :] = jnp.full((1, 128), blocks_ref[e, k, 0, d])
    mine = jnp.where(lax.axis_index("cond") == 0, weights_ref[0], weights_ref[1])
    total = weights_ref[0].astype(jnp.float32) + weights_ref[1].astype(jnp.float32)
    one = jnp.ones((1, 128), jnp.float32)
    last = 6 * nvar * nvar
    table_ref[last : last + 1, :] = (one * mine.astype(jnp.float32)) / (one * total)
    for copy in copies[2:]:
        copy.wait()
    write_sides(lambda k, x: v_ref[k, x], nvar, nx, ny, xa_ref, xb_ref, ya_ref, yb_ref)
    even = lax.rem(position()[1], 2) == 0
    for x in range(nx):
        here = slice(x, x + 1)
        yb_ref[2 * nvar, here, :] = jnp.where(even, diagonal_ref[x, 0:1], diagonal_ref[x, ny - 1 : ny])
        for k in range(nvar):
            next_ref[k, here, :] = jnp.where(even, v_ref[k, x, 1:2], v_ref[k, x, ny - 2 : ny - 1])
            wanted_ref[k, here, :] = jnp.where(even, source_ref[k, x, 0:1], source_ref[k, x, ny - 1 : ny])
    row = lax.broadcasted_iota(jnp.int32, (nx, nz), 0)
    lane = lax.broadcasted_iota(jnp.int32, (nx, nz), 1)
    sums = [0.0] * nvar
    for e in range(nvar):
        edge = yb_ref[e]
        shifted = {
            0: jnp.where(row == nx - 1, 0.0, pltpu.roll(edge, nx - 1, 0)),
            1: jnp.where(row == 0, 0.0, pltpu.roll(edge, 1, 0)),
            4: jnp.where(lane == nz - 1, 0.0, pltpu.roll(edge, nz - 1, 1)),
            5: jnp.where(lane == 0, 0.0, pltpu.roll(edge, 1, 1)),
        }
        inward = next_ref[e]
        for k in range(nvar):
            for d, values in shifted.items():
                sums[k] = sums[k] + coefficient(table_ref, d, e, k, nvar, values.shape) * values
            both = [coefficient(table_ref, d, e, k, nvar, inward.shape) for d in (2, 3)]
            sums[k] = sums[k] + jnp.where(even, both[0], both[1]) * inward
    diagonal = yb_ref[2 * nvar]
    scale = RELAXATION / diagonal
    for k in range(nvar):
        edge = yb_ref[k]
        yb_ref[nvar + k] = edge + scale * (wanted_ref[k] - diagonal * edge + sums[k])
    yb_ref[2 * nvar] = scale


def neighbour_sums(v_ref, blocks_ref, x):
    nvar, nx, ny, nz = v_ref.shape
    row = lax.broadcasted_iota(jnp.int32, (ny, nz), 0)
    lane = lax.broadcasted_iota(jnp.int32, (ny, nz), 1)
    sums = [None] * nvar
    for e in range(nvar):
        centre = v_ref[e, x]
        shifted = {}
        if x + 1 < nx:
            shifted[0] = v_ref[e, x + 1]
        if x > 0:
            shifted[1] = v_ref[e, x - 1]
        shifted[2] = jnp.where(row == ny - 1, 0.0, pltpu.roll(centre, ny - 1, 0))
        shifted[3] = jnp.where(row == 0, 0.0, pltpu.roll(centre, 1, 0))
        shifted[4] = jnp.where(lane == nz - 1, 0.0, pltpu.roll(centre, nz - 1, 1))
        shifted[5] = jnp.where(lane == 0, 0.0, pltpu.roll(centre, 1, 1))
        for d, values in shifted.items():
            for k in range(nvar):
                term = coefficient(blocks_ref, d, e, k, nvar, values.shape) * values
                sums[k] = term if sums[k] is None else sums[k] + term
    return sums


def inner_sweep_kernel(blocks_ref, v_ref, source_ref, diagonal_ref, out_ref):
    nvar, nx, _, _ = v_ref.shape
    for x in range(nx):
        sums = neighbour_sums(v_ref, blocks_ref, x)
        diagonal = diagonal_ref[x]
        scale = RELAXATION / diagonal
        for k in range(nvar):
            value = v_ref[k, x]
            out_ref[k, x] = value + scale * (source_ref[k, x] - diagonal * value + sums[k])


def inner_residual_kernel(blocks_ref, v_ref, source_ref, diagonal_ref, out_ref, v_hbm, sem):
    copy = pltpu.make_async_copy(v_ref, v_hbm, sem)
    copy.start()
    nvar, nx, _, _ = v_ref.shape
    for x in range(nx):
        sums = neighbour_sums(v_ref, blocks_ref, x)
        diagonal = diagonal_ref[x]
        for k in range(nvar):
            out_ref[k, x] = source_ref[k, x] - diagonal * v_ref[k, x] + sums[k]
    copy.wait()


def add_halo(blocks_ref, inner_ref, diagonal_ref, xa, xb, ya, yb, out_ref):
    nvar, nx, ny, nz = inner_ref.shape
    gx, yz = position()
    gx_even, yz_even = lax.rem(gx, 2) == 0, lax.rem(yz, 2) == 0
    has_low_x, has_high_x = gx > 0, gx < 7
    has_low_y, has_high_y = yz > 0, yz < 15

    def halo_sums(direction, pick):
        sums = [None] * nvar
        for e in range(nvar):
            values = pick(e)
            for k in range(nvar):
                term = coefficient(blocks_ref, direction, e, k, nvar, values.shape) * values
                sums[k] = term if sums[k] is None else sums[k] + term
        return sums

    def picker(even, a, b, exists):
        return lambda e: jnp.where(exists, jnp.where(even, a(e), b(e)), 0.0)

    high_y = halo_sums(2, picker(yz_even, ya, yb, has_high_y))
    low_y = halo_sums(3, picker(yz_even, yb, ya, has_low_y))
    row = lax.broadcasted_iota(jnp.int32, (8, nz), 0)
    for x in range(nx):
        if x == 0:
            at_x = halo_sums(1, picker(gx_even, xb, xa, has_low_x))
        elif x == nx - 1:
            at_x = halo_sums(0, picker(gx_even, xa, xb, has_high_x))
        else:
            at_x = None
        for start in range(0, ny, 8):
            rows = slice(start, start + 8)
            scale = None if diagonal_ref is None else RELAXATION / diagonal_ref[x, rows]
            for k in range(nvar):
                more = None
                if start == 0:
                    more = jnp.where(row == 0, low_y[k][x : x + 1], 0.0)
                if start == ny - 8:
                    last = jnp.where(row == 7, high_y[k][x : x + 1], 0.0)
                    more = last if more is None else more + last
                if at_x is not None:
                    more = at_x[k][rows] if more is None else more + at_x[k][rows]
                value = inner_ref[k, x, rows]
                if more is not None:
                    value = value + (more if scale is None else scale * more)
                out_ref[k, x, rows] = value


def reader(ref):
    return lambda e: ref[e]


def outer_sweep_kernel(
    blocks_ref, inner_ref, diagonal_ref, xa_ref, xb_ref, ya_ref, yb_ref,
    out_ref, next_xa_ref, next_xb_ref, next_ya_ref,
):
    nvar, nx, ny, nz = inner_ref.shape
    halo = [reader(ref) for ref in (xa_ref, xb_ref, ya_ref, yb_ref)]
    add_halo(blocks_ref, inner_ref, diagonal_ref, *halo, out_ref)
    gx, yz = position()
    gx_even, yz_even = lax.rem(gx, 2) == 0, lax.rem(yz, 2) == 0
    top = nvar * ny
    next_xa_ref[top:, :] = jnp.zeros((next_xa_ref.shape[0] - top, nz), jnp.float32)
    next_xb_ref[top:, :] = jnp.zeros((next_xb_ref.shape[0] - top, nz), jnp.float32)
    for k in range(nvar):
        low, high = out_ref[k, 0], out_ref[k, nx - 1]
        next_xa_ref[k * ny : (k + 1) * ny, :] = jnp.where(gx_even, high, low)
        next_xb_ref[k * ny : (k + 1) * ny, :] = jnp.where(gx_even, low, high)
        low, high = yb_ref[k, 0:1], yb_ref[k, nx - 1 : nx]
        next_xa_ref[top + k : top + k + 1, :] = jnp.where(gx_even, high, low)
        next_xb_ref[top + k : top + k + 1, :] = jnp.where(gx_even, low, high)
        for x in range(nx):
            slab = out_ref[k, x]
            next_ya_ref[k, x : x + 1, :] = jnp.where(yz_even, slab[ny - 1 : ny], slab[0:1])


def complete_far_row(blocks_ref, xa_ref, xb_ref, far_ref, edge_ref, out_ref):
    nvar, nx, nz = out_ref.shape
    top = xa_ref.shape[0] - 8
    gx, yz = position()
    gx_even, yz_even = lax.rem(gx, 2) == 0, lax.rem(yz, 2) == 0
    row = lax.broadcasted_iota(jnp.int32, (nx, nz), 0)
    at_low, at_high = (row == 0) & (gx > 0), (row == nx - 1) & (gx < 7)
    sums = [0.0] * nvar
    for e in range(nvar):
        edge = edge_ref[e]
        a, b = xa_ref[top + e : top + e + 1, :], xb_ref[top + e : top + e + 1, :]
        low = jnp.where(at_low, jnp.where(gx_even, b, a), 0.0)
        high = jnp.where(at_high, jnp.where(gx_even, a, b), 0.0)
        for k in range(nvar):
            both = [coefficient(blocks_ref, d, e, k, nvar, edge.shape) for d in (2, 3)]
            sums[k] = sums[k] + jnp.where(yz_even, both[0], both[1]) * edge
            sums[k] = sums[k] + coefficient(blocks_ref, 1, e, k, nvar, edge.shape) * low
            sums[k] = sums[k] + coefficient(blocks_ref, 0, e, k, nvar, edge.shape) * high
    for k in range(nvar):
        out_ref[k] = far_ref[nvar + k] + far_ref[2 * nvar] * sums[k]


def last_sweep_kernel(
    blocks_ref, inner_ref, diagonal_ref, xa_ref, xb_ref, ya_ref, far_ref, edge_ref,
    sensitivity_ref, mask_ref, slot_ref, basis_ref,
    out_ref, next_xa_ref, next_xb_ref, next_ya_ref, next_yb_ref, gradient_ref, surface_ref, row_ref,
):
    nvar, nx, ny, _ = inner_ref.shape
    complete_far_row(blocks_ref, xa_ref, xb_ref, far_ref, edge_ref, row_ref)
    add_halo(
        blocks_ref, inner_ref, diagonal_ref,
        lambda e: xa_ref[e * ny : (e + 1) * ny, :],
        lambda e: xb_ref[e * ny : (e + 1) * ny, :],
        reader(ya_ref), reader(row_ref), out_ref,
    )
    write_sides(
        lambda k, x: out_ref[k, x], nvar, nx, ny, next_xa_ref, next_xb_ref, next_ya_ref, next_yb_ref
    )
    nvar, nx, ny, _ = inner_ref.shape
    for x in range(nx):
        total = out_ref[0, x] * sensitivity_ref[0, x].astype(jnp.float32)
        for k in range(1, nvar):
            total = total + out_ref[k, x] * sensitivity_ref[k, x].astype(jnp.float32)
        surface_ref[x * ny : (x + 1) * ny, :] = mask_ref[x].astype(jnp.float32) * total
    projected = jnp.dot(
        surface_ref[...], basis_ref[...], precision=HIGHEST, preferred_element_type=jnp.float32
    )
    patches, band = projected.shape
    half = band // 2
    pairs = NDES // band
    wanted = lax.broadcasted_iota(jnp.int32, (2 * pairs, patches), 0)
    wanted = jnp.where(wanted < pairs, 2 * wanted, 2 * (wanted - pairs) + 1)
    lane = lax.broadcasted_iota(jnp.int32, (ny, patches), 1)
    repeat = lax.rem(lane, ny) == lax.broadcasted_iota(jnp.int32, (ny, patches), 0)
    slots = jnp.dot(
        slot_ref[...].astype(jnp.float32), repeat.astype(jnp.float32), preferred_element_type=jnp.float32
    )
    lane = lax.broadcasted_iota(jnp.int32, (nx, patches), 1)
    own = lax.div(lane, ny) == lax.broadcasted_iota(jnp.int32, (nx, patches), 0)
    slots = jnp.sum(jnp.where(own, slots, 0.0), axis=0, keepdims=True)
    onehot = (wanted.astype(jnp.float32) == slots).astype(jnp.float32)
    by_slot = jnp.dot(onehot, projected, precision=HIGHEST, preferred_element_type=jnp.float32)
    even, odd = by_slot[:pairs], pltpu.roll(by_slot[pairs:], half, 1)
    row = lax.broadcasted_iota(jnp.int32, (pairs, band), 0)
    lane = lax.broadcasted_iota(jnp.int32, (pairs, band), 1)
    before = jnp.where(row == 0, 0.0, pltpu.roll(odd, 1, 0))
    gradient = even + jnp.where(lane < half, before, odd)
    share = blocks_ref[pl.ds(6 * nvar * nvar, 8, stride=0), :]
    gradient_ref[...] = gradient * jnp.concatenate([share] * (pairs // 8), axis=0)


def outer_residual_kernel(blocks_ref, inner_ref, xa_ref, xb_ref, ya_ref, yb_ref, out_ref):
    halo = [reader(ref) for ref in (xa_ref, xb_ref, ya_ref, yb_ref)]
    add_halo(blocks_ref, inner_ref, None, *halo, out_ref)


def finish_kernel(part_ref, other_ref, piece_ref):
    size = piece_ref.shape[1]
    total = part_ref[...] + other_ref[...]
    which = lax.axis_index("yz_1")
    piece = total[:, :size]
    for i in range(1, total.shape[1] // size):
        piece = jnp.where(which == i, total[:, i * size : (i + 1) * size], piece)
    piece_ref[...] = piece


def swap_a(n):
    return [(i, i ^ 1) for i in range(n)]


def swap_b(n):
    return [(i, (((i + 1) ^ 1) - 1) % n) for i in range(n)]


def exchange(xa, xb, ya, yb=None):
    far = [] if yb is None else [lax.ppermute(yb, YZ, swap_b(16))]
    chip = lax.ppermute(xb, GX, swap_b(8))
    core = lax.ppermute(xa, GX, swap_a(8))
    near = lax.ppermute(ya, YZ, swap_a(16))
    return [near_core(x) for x in (core, chip, near, *far)]


def step(
    adjoint,
    objective_gradient,
    diagonal,
    flux_blocks,
    flux_sensitivity,
    surface_mask,
    patch_band_slot,
    design_basis,
    condition_weights,
):
    sensitivity, mask = near_core(flux_sensitivity[0]), near_core(surface_mask)
    basis = near_core(design_basis)
    _, nvar, nx, ny, nz = adjoint.shape
    field = kept(nvar, nx, ny, nz)
    sides = (kept(nvar, ny, nz), kept(nvar, ny, nz), kept(nvar, nx, nz), kept(nvar, nx, nz))

    arrays = (flux_blocks.transpose(2, 3, 0, 1), condition_weights, adjoint[0], objective_gradient[0], diagonal)
    v, source, diagonal, blocks, *first = call(
        load_kernel,
        out_shape=(
            field,
            field,
            kept(nx, ny, nz),
            kept(6 * nvar * nvar + 1, 128),
            *sides[:3],
            kept(2 * nvar + 1, nx, nz),
        ),
        in_specs=[HBM] * 5,
        out_specs=[VMEM] * 8,
        scratch_shapes=[
            pltpu.SMEM((nvar, nvar, 1, 6), jnp.float32),
            pltpu.SMEM(condition_weights.shape, jnp.int32),
            pltpu.VMEM((nvar, nx, nz), jnp.float32),
            pltpu.VMEM((nvar, nx, nz), jnp.float32),
            pltpu.SemaphoreType.DMA((5,)),
        ],
        name="load",
    )(*(far_from_core(x) for x in arrays))
    v, source, diagonal, blocks = (near_core(x) for x in (v, source, diagonal, blocks))
    halo = exchange(*first)
    inner_sweep = call(
        inner_sweep_kernel, out_shape=field, in_specs=[VMEM] * 4, out_specs=VMEM, name="inner_sweep"
    )
    inner = inner_sweep(blocks, v, source, diagonal)
    relaxed, *second = call(
        outer_sweep_kernel,
        out_shape=(field, kept(nvar * ny + 8, nz), kept(nvar * ny + 8, nz), sides[2]),
        in_specs=[VMEM] * 7,
        out_specs=[VMEM] * 4,
        name="outer_sweep",
    )(blocks, near_core(inner), diagonal, *halo)
    far, edge = halo[3], near_core(first[3])

    halo = exchange(*second)
    inner = inner_sweep(blocks, near_core(relaxed), source, diagonal)
    smoothed, xa, xb, ya, yb, gradient = call(
        last_sweep_kernel,
        out_shape=(field, *sides, kept(NDES // 128, 128)),
        in_specs=[VMEM] * 12,
        out_specs=[VMEM] * 6,
        scratch_shapes=[
            pltpu.VMEM((nx * ny, nz), jnp.float32),
            pltpu.VMEM((nvar, nx, nz), jnp.float32),
        ],
        name="last_sweep",
    )(
        blocks, near_core(inner), diagonal, *halo, far, edge,
        sensitivity, mask, near_core(patch_band_slot), basis,
    )

    parts = lax.all_to_all(gradient, SPREAD, 0, 0, tiled=True)
    total = jnp.sum(parts, axis=0, keepdims=True)
    total = total + lax.ppermute(total, RING, [(i, i ^ 1) for i in range(8)])
    halo = exchange(xa, xb, ya, yb)
    total = total + lax.ppermute(total, RING, [(i, (((i + 1) ^ 1) - 1) % 8) for i in range(8)])
    across = [(0, 3), (3, 0), (1, 6), (6, 1), (2, 5), (5, 2), (4, 7), (7, 4)]
    other = lax.ppermute(total, RING, across)

    inner, smoothed = call(
        inner_residual_kernel,
        out_shape=(field, pltpu.HBM((nvar, nx, ny, nz), jnp.float32)),
        in_specs=[VMEM] * 4,
        out_specs=[VMEM, HBM],
        scratch_shapes=[pltpu.SemaphoreType.DMA],
        name="inner_residual",
    )(blocks, near_core(smoothed), source, diagonal)
    residual = call(
        outer_residual_kernel,
        out_shape=f32(nvar, nx, ny, nz),
        in_specs=[VMEM] * 6,
        out_specs=VMEM,
        name="outer_residual",
    )(blocks, near_core(inner), *halo)
    design_gradient = call(
        finish_kernel, out_shape=f32(1, 32), in_specs=[VMEM] * 2, out_specs=VMEM, name="finish"
    )(near_core(total), near_core(other))
    return smoothed[None], residual[None], design_gradient.reshape(-1)


def solution(mesh):
    torus = Mesh(
        mesh.devices.reshape(mesh.shape["cond"], 4, 2, 4, 4),
        ("cond", "gx_0", "gx_1", "yz_0", "yz_1"),
    )
    in_specs = (
        P("cond", None, GX, YZ, None),
        P("cond", None, GX, YZ, None),
        P(GX, YZ, None),
        P("cond", None, None, None),
        P("cond", None, GX, YZ, None),
        P(GX, YZ, None),
        P(GX, YZ),
        P(),
        P(),
    )
    out_specs = (P("cond", None, GX, YZ, None), P("cond", None, GX, YZ, None), P(GX + YZ))
    return jax.shard_map(step, mesh=torus, in_specs=in_specs, out_specs=out_specs, check_vma=False)
```

```python
import jax
import jax.numpy as jnp
from jax import lax
from jax.experimental import pallas as pl
from jax.experimental.pallas import tpu as pltpu
from jax.sharding import Mesh
from jax.sharding import PartitionSpec as P


NDES = 4096
GX = ("gx_0", "gx_1")
YZ = ("yz_0", "yz_1")
RING = ("cond", "yz_1")
SPREAD = ("gx_0", "gx_1", "yz_0")
RELAXATION = 0.8
HIGHEST = lax.Precision.HIGHEST

VMEM = pl.BlockSpec(memory_space=pltpu.VMEM)
HBM = pl.BlockSpec(memory_space=pltpu.HBM)
SMEM = pl.BlockSpec(memory_space=pltpu.SMEM)


def f32(*shape):
    return jax.ShapeDtypeStruct(shape, jnp.float32)


def kept(*shape):
    return pltpu.VMEM(shape, jnp.float32)


def far_from_core(x):
    return pltpu.with_memory_space_constraint(x, pltpu.HBM)


def near_core(x):
    return pltpu.with_memory_space_constraint(x, pltpu.VMEM)


def call(kernel, **options):
    params = pltpu.CompilerParams(vmem_limit_bytes=8 * 2**20)
    return pl.pallas_call(kernel, compiler_params=params, **options)


def position():
    gx = lax.axis_index("gx_0") * 2 + lax.axis_index("gx_1")
    yz = lax.axis_index("yz_0") * 4 + lax.axis_index("yz_1")
    return gx, yz


def write_sides(read, nvar, nx, ny, xa_ref, xb_ref, ya_ref, yb_ref):
    gx, yz = position()
    gx_even, yz_even = lax.rem(gx, 2) == 0, lax.rem(yz, 2) == 0
    for k in range(nvar):
        low, high = read(k, 0), read(k, nx - 1)
        xa_ref[k] = jnp.where(gx_even, high, low)
        xb_ref[k] = jnp.where(gx_even, low, high)
        for x in range(nx):
            slab = read(k, x)
            first, last = slab[0:1], slab[ny - 1 : ny]
            ya_ref[k, x : x + 1, :] = jnp.where(yz_even, last, first)
            yb_ref[k, x : x + 1, :] = jnp.where(yz_even, first, last)


def coefficient(table_ref, d, e, k, nvar, shape):
    tile = table_ref[pl.ds((d * nvar + e) * nvar + k, 8, stride=0), :]
    rows = jnp.concatenate([tile] * (shape[0] // 8), axis=0)
    return jnp.concatenate([rows] * (shape[1] // 128), axis=1)


def load_kernel(
    blocks_hbm, weights_hbm, v_hbm, source_hbm, diagonal_hbm,
    v_ref, source_ref, diagonal_ref, table_ref, yb_ref,
    blocks_ref, weights_ref, next_ref, wanted_ref, sems,
):
    pairs = (
        (blocks_hbm, blocks_ref),
        (weights_hbm, weights_ref),
        (v_hbm, v_ref),
        (source_hbm, source_ref),
        (diagonal_hbm, diagonal_ref),
    )
    copies = [pltpu.make_async_copy(a, b, sems.at[i]) for i, (a, b) in enumerate(pairs)]
    for copy in copies:
        copy.start()
    nvar, _, _, _ = v_ref.shape
    for copy in copies[:2]:
        copy.wait()
    for d in range(6):
        for e in range(nvar):
            for k in range(nvar):
                row = (d * nvar + e) * nvar + k
                table_ref[row : row + 1, :] = jnp.full((1, 128), blocks_ref[e, k, 0, d])
    mine = jnp.where(lax.axis_index("cond") == 0, weights_ref[0], weights_ref[1])
    total = weights_ref[0].astype(jnp.float32) + weights_ref[1].astype(jnp.float32)
    one = jnp.ones((1, 128), jnp.float32)
    last = 6 * nvar * nvar
    table_ref[last : last + 1, :] = (one * mine.astype(jnp.float32)) / (one * total)
    for copy in copies[2:]:
        copy.wait()
    even = lax.rem(position()[1], 2) == 0
    relax_edge(table_ref, v_ref, source_ref, diagonal_ref, even, yb_ref, next_ref, wanted_ref)


def other_sides_kernel(
    table_ref, v_ref, source_ref, diagonal_ref, xa_ref, xb_ref, ya_ref, next_ref, wanted_ref
):
    nvar, nx, _, _ = v_ref.shape
    gx, yz = position()
    gx_even, yz_even = lax.rem(gx, 2) == 0, lax.rem(yz, 2) == 0
    for k in range(nvar):
        low, high = v_ref[k, 0], v_ref[k, nx - 1]
        xa_ref[k] = jnp.where(gx_even, high, low)
        xb_ref[k] = jnp.where(gx_even, low, high)
    relax_edge(table_ref, v_ref, source_ref, diagonal_ref, ~yz_even, ya_ref, next_ref, wanted_ref)


def relax_edge(table_ref, v_ref, source_ref, diagonal_ref, is_low, out_ref, next_ref, wanted_ref):
    nvar, nx, ny, nz = v_ref.shape
    for x in range(nx):
        here = slice(x, x + 1)
        out_ref[2 * nvar, here, :] = jnp.where(is_low, diagonal_ref[x, 0:1], diagonal_ref[x, ny - 1 : ny])
        for k in range(nvar):
            out_ref[k, here, :] = jnp.where(is_low, v_ref[k, x, 0:1], v_ref[k, x, ny - 1 : ny])
            next_ref[k, here, :] = jnp.where(is_low, v_ref[k, x, 1:2], v_ref[k, x, ny - 2 : ny - 1])
            wanted_ref[k, here, :] = jnp.where(is_low, source_ref[k, x, 0:1], source_ref[k, x, ny - 1 : ny])
    row = lax.broadcasted_iota(jnp.int32, (nx, nz), 0)
    lane = lax.broadcasted_iota(jnp.int32, (nx, nz), 1)
    sums = [0.0] * nvar
    for e in range(nvar):
        edge = out_ref[e]
        shifted = {
            0: jnp.where(row == nx - 1, 0.0, pltpu.roll(edge, nx - 1, 0)),
            1: jnp.where(row == 0, 0.0, pltpu.roll(edge, 1, 0)),
            4: jnp.where(lane == nz - 1, 0.0, pltpu.roll(edge, nz - 1, 1)),
            5: jnp.where(lane == 0, 0.0, pltpu.roll(edge, 1, 1)),
        }
        inward = next_ref[e]
        for k in range(nvar):
            for d, values in shifted.items():
                sums[k] = sums[k] + coefficient(table_ref, d, e, k, nvar, values.shape) * values
            both = [coefficient(table_ref, d, e, k, nvar, inward.shape) for d in (2, 3)]
            sums[k] = sums[k] + jnp.where(is_low, both[0], both[1]) * inward
    diagonal = out_ref[2 * nvar]
    scale = RELAXATION / diagonal
    for k in range(nvar):
        edge = out_ref[k]
        out_ref[nvar + k] = edge + scale * (wanted_ref[k] - diagonal * edge + sums[k])
    out_ref[2 * nvar] = scale


def neighbour_sums(v_ref, blocks_ref, x):
    nvar, nx, ny, nz = v_ref.shape
    row = lax.broadcasted_iota(jnp.int32, (ny, nz), 0)
    lane = lax.broadcasted_iota(jnp.int32, (ny, nz), 1)
    sums = [None] * nvar
    for e in range(nvar):
        centre = v_ref[e, x]
        shifted = {}
        if x + 1 < nx:
            shifted[0] = v_ref[e, x + 1]
        if x > 0:
            shifted[1] = v_ref[e, x - 1]
        shifted[2] = jnp.where(row == ny - 1, 0.0, pltpu.roll(centre, ny - 1, 0))
        shifted[3] = jnp.where(row == 0, 0.0, pltpu.roll(centre, 1, 0))
        shifted[4] = jnp.where(lane == nz - 1, 0.0, pltpu.roll(centre, nz - 1, 1))
        shifted[5] = jnp.where(lane == 0, 0.0, pltpu.roll(centre, 1, 1))
        for d, values in shifted.items():
            for k in range(nvar):
                term = coefficient(blocks_ref, d, e, k, nvar, values.shape) * values
                sums[k] = term if sums[k] is None else sums[k] + term
    return sums


def inner_sweep_kernel(blocks_ref, v_ref, source_ref, diagonal_ref, out_ref):
    nvar, nx, _, _ = v_ref.shape
    for x in range(nx):
        sums = neighbour_sums(v_ref, blocks_ref, x)
        diagonal = diagonal_ref[x]
        scale = RELAXATION / diagonal
        for k in range(nvar):
            value = v_ref[k, x]
            out_ref[k, x] = value + scale * (source_ref[k, x] - diagonal * value + sums[k])


def inner_residual_kernel(blocks_ref, v_ref, source_ref, diagonal_ref, out_ref, v_hbm, sem):
    copy = pltpu.make_async_copy(v_ref, v_hbm, sem)
    copy.start()
    nvar, nx, _, _ = v_ref.shape
    for x in range(nx):
        sums = neighbour_sums(v_ref, blocks_ref, x)
        diagonal = diagonal_ref[x]
        for k in range(nvar):
            out_ref[k, x] = source_ref[k, x] - diagonal * v_ref[k, x] + sums[k]
    copy.wait()


def add_halo(blocks_ref, inner_ref, diagonal_ref, xa, xb, ya, yb, out_ref):
    nvar, nx, ny, nz = inner_ref.shape
    gx, yz = position()
    gx_even, yz_even = lax.rem(gx, 2) == 0, lax.rem(yz, 2) == 0
    has_low_x, has_high_x = gx > 0, gx < 7
    has_low_y, has_high_y = yz > 0, yz < 15

    def halo_sums(direction, pick):
        sums = [None] * nvar
        for e in range(nvar):
            values = pick(e)
            for k in range(nvar):
                term = coefficient(blocks_ref, direction, e, k, nvar, values.shape) * values
                sums[k] = term if sums[k] is None else sums[k] + term
        return sums

    def picker(even, a, b, exists):
        return lambda e: jnp.where(exists, jnp.where(even, a(e), b(e)), 0.0)

    high_y = halo_sums(2, picker(yz_even, ya, yb, has_high_y))
    low_y = halo_sums(3, picker(yz_even, yb, ya, has_low_y))
    row = lax.broadcasted_iota(jnp.int32, (8, nz), 0)
    for x in range(nx):
        if x == 0:
            at_x = halo_sums(1, picker(gx_even, xb, xa, has_low_x))
        elif x == nx - 1:
            at_x = halo_sums(0, picker(gx_even, xa, xb, has_high_x))
        else:
            at_x = None
        for start in range(0, ny, 8):
            rows = slice(start, start + 8)
            scale = None if diagonal_ref is None else RELAXATION / diagonal_ref[x, rows]
            for k in range(nvar):
                more = None
                if start == 0:
                    more = jnp.where(row == 0, low_y[k][x : x + 1], 0.0)
                if start == ny - 8:
                    last = jnp.where(row == 7, high_y[k][x : x + 1], 0.0)
                    more = last if more is None else more + last
                if at_x is not None:
                    more = at_x[k][rows] if more is None else more + at_x[k][rows]
                value = inner_ref[k, x, rows]
                if more is not None:
                    value = value + (more if scale is None else scale * more)
                out_ref[k, x, rows] = value


def reader(ref):
    return lambda e: ref[e]


def outer_sweep_kernel(
    blocks_ref, inner_ref, diagonal_ref, xa_ref, xb_ref, ya_ref, yb_ref, out_ref, next_xa_ref, next_xb_ref,
):
    nvar, nx, ny, nz = inner_ref.shape
    halo = [reader(ref) for ref in (xa_ref, xb_ref, ya_ref, yb_ref)]
    add_halo(blocks_ref, inner_ref, diagonal_ref, *halo, out_ref)
    gx_even = lax.rem(position()[0], 2) == 0
    top = nvar * ny
    next_xa_ref[top:, :] = jnp.zeros((next_xa_ref.shape[0] - top, nz), jnp.float32)
    next_xb_ref[top:, :] = jnp.zeros((next_xb_ref.shape[0] - top, nz), jnp.float32)
    for k in range(nvar):
        low, high = out_ref[k, 0], out_ref[k, nx - 1]
        next_xa_ref[k * ny : (k + 1) * ny, :] = jnp.where(gx_even, high, low)
        next_xb_ref[k * ny : (k + 1) * ny, :] = jnp.where(gx_even, low, high)
        for start, ref in ((top, ya_ref), (top + nvar, yb_ref)):
            low, high = ref[k, 0:1], ref[k, nx - 1 : nx]
            next_xa_ref[start + k : start + k + 1, :] = jnp.where(gx_even, high, low)
            next_xb_ref[start + k : start + k + 1, :] = jnp.where(gx_even, low, high)


def complete_row(blocks_ref, xa_ref, xb_ref, top, is_low, far_ref, edge_ref, out_ref):
    nvar, nx, nz = out_ref.shape
    gx = position()[0]
    gx_even = lax.rem(gx, 2) == 0
    row = lax.broadcasted_iota(jnp.int32, (nx, nz), 0)
    at_low, at_high = (row == 0) & (gx > 0), (row == nx - 1) & (gx < 7)
    sums = [0.0] * nvar
    for e in range(nvar):
        edge = edge_ref[e]
        a, b = xa_ref[top + e : top + e + 1, :], xb_ref[top + e : top + e + 1, :]
        low = jnp.where(at_low, jnp.where(gx_even, b, a), 0.0)
        high = jnp.where(at_high, jnp.where(gx_even, a, b), 0.0)
        for k in range(nvar):
            both = [coefficient(blocks_ref, d, e, k, nvar, edge.shape) for d in (2, 3)]
            sums[k] = sums[k] + jnp.where(is_low, both[0], both[1]) * edge
            sums[k] = sums[k] + coefficient(blocks_ref, 1, e, k, nvar, edge.shape) * low
            sums[k] = sums[k] + coefficient(blocks_ref, 0, e, k, nvar, edge.shape) * high
    for k in range(nvar):
        out_ref[k] = far_ref[nvar + k] + far_ref[2 * nvar] * sums[k]


def last_sweep_kernel(
    blocks_ref, inner_ref, diagonal_ref, xa_ref, xb_ref, ya_ref, yb_ref, sent_ya_ref, sent_yb_ref,
    sensitivity_ref, mask_ref, slot_ref, basis_ref,
    out_ref, next_xa_ref, next_xb_ref, next_ya_ref, next_yb_ref, gradient_ref, surface_ref, row_a_ref, row_b_ref,
):
    nvar, nx, ny, _ = inner_ref.shape
    even, top = lax.rem(position()[1], 2) == 0, nvar * ny
    complete_row(blocks_ref, xa_ref, xb_ref, top, ~even, ya_ref, sent_ya_ref, row_a_ref)
    complete_row(blocks_ref, xa_ref, xb_ref, top + nvar, even, yb_ref, sent_yb_ref, row_b_ref)
    add_halo(
        blocks_ref, inner_ref, diagonal_ref,
        lambda e: xa_ref[e * ny : (e + 1) * ny, :],
        lambda e: xb_ref[e * ny : (e + 1) * ny, :],
        reader(row_a_ref), reader(row_b_ref), out_ref,
    )
    write_sides(
        lambda k, x: out_ref[k, x], nvar, nx, ny, next_xa_ref, next_xb_ref, next_ya_ref, next_yb_ref
    )
    nvar, nx, ny, _ = inner_ref.shape
    for x in range(nx):
        total = out_ref[0, x] * sensitivity_ref[0, x].astype(jnp.float32)
        for k in range(1, nvar):
            total = total + out_ref[k, x] * sensitivity_ref[k, x].astype(jnp.float32)
        surface_ref[x * ny : (x + 1) * ny, :] = mask_ref[x].astype(jnp.float32) * total
    projected = jnp.dot(
        surface_ref[...], basis_ref[...], precision=HIGHEST, preferred_element_type=jnp.float32
    )
    patches, band = projected.shape
    half = band // 2
    pairs = NDES // band
    wanted = lax.broadcasted_iota(jnp.int32, (2 * pairs, patches), 0)
    wanted = jnp.where(wanted < pairs, 2 * wanted, 2 * (wanted - pairs) + 1)
    lane = lax.broadcasted_iota(jnp.int32, (ny, patches), 1)
    repeat = lax.rem(lane, ny) == lax.broadcasted_iota(jnp.int32, (ny, patches), 0)
    slots = jnp.dot(
        slot_ref[...].astype(jnp.float32), repeat.astype(jnp.float32), preferred_element_type=jnp.float32
    )
    lane = lax.broadcasted_iota(jnp.int32, (nx, patches), 1)
    own = lax.div(lane, ny) == lax.broadcasted_iota(jnp.int32, (nx, patches), 0)
    slots = jnp.sum(jnp.where(own, slots, 0.0), axis=0, keepdims=True)
    onehot = (wanted.astype(jnp.float32) == slots).astype(jnp.float32)
    by_slot = jnp.dot(onehot, projected, precision=HIGHEST, preferred_element_type=jnp.float32)
    even, odd = by_slot[:pairs], pltpu.roll(by_slot[pairs:], half, 1)
    row = lax.broadcasted_iota(jnp.int32, (pairs, band), 0)
    lane = lax.broadcasted_iota(jnp.int32, (pairs, band), 1)
    before = jnp.where(row == 0, 0.0, pltpu.roll(odd, 1, 0))
    gradient = even + jnp.where(lane < half, before, odd)
    share = blocks_ref[pl.ds(6 * nvar * nvar, 8, stride=0), :]
    gradient_ref[...] = gradient * jnp.concatenate([share] * (pairs // 8), axis=0)


def outer_residual_kernel(blocks_ref, inner_ref, xa_ref, xb_ref, ya_ref, yb_ref, out_ref):
    halo = [reader(ref) for ref in (xa_ref, xb_ref, ya_ref, yb_ref)]
    add_halo(blocks_ref, inner_ref, None, *halo, out_ref)


def swap_a(n):
    return [(i, i ^ 1) for i in range(n)]


def swap_b(n):
    return [(i, (((i + 1) ^ 1) - 1) % n) for i in range(n)]


def exchange(xa, xb, ya=None, yb=None):
    far = [] if yb is None else [lax.ppermute(yb, YZ, swap_b(16))]
    near = [] if ya is None else [lax.ppermute(ya, YZ, swap_a(16))]
    chip = lax.ppermute(xb, GX, swap_b(8))
    core = lax.ppermute(xa, GX, swap_a(8))
    return [near_core(x) for x in (core, chip, *near, *far)]


def step(
    adjoint,
    objective_gradient,
    diagonal,
    flux_blocks,
    flux_sensitivity,
    surface_mask,
    patch_band_slot,
    design_basis,
    condition_weights,
):
    sensitivity, mask = near_core(flux_sensitivity[0]), near_core(surface_mask)
    basis = near_core(design_basis)
    _, nvar, nx, ny, nz = adjoint.shape
    field = kept(nvar, nx, ny, nz)
    sides = (kept(nvar, ny, nz), kept(nvar, ny, nz), kept(nvar, nx, nz), kept(nvar, nx, nz))

    arrays = (flux_blocks.transpose(2, 3, 0, 1), condition_weights, adjoint[0], objective_gradient[0], diagonal)
    row = kept(2 * nvar + 1, nx, nz)
    rows_scratch = [pltpu.VMEM((nvar, nx, nz), jnp.float32)] * 2
    v, source, diagonal, blocks, yb = call(
        load_kernel,
        out_shape=(field, field, kept(nx, ny, nz), kept(6 * nvar * nvar + 1, 128), row),
        in_specs=[HBM] * 5,
        out_specs=[VMEM] * 5,
        scratch_shapes=[
            pltpu.SMEM((nvar, nvar, 1, 6), jnp.float32),
            pltpu.SMEM(condition_weights.shape, jnp.int32),
            *rows_scratch,
            pltpu.SemaphoreType.DMA((5,)),
        ],
        name="load",
    )(*(far_from_core(x) for x in arrays))
    v, source, diagonal, blocks = (near_core(x) for x in (v, source, diagonal, blocks))
    xa, xb, ya = call(
        other_sides_kernel,
        out_shape=(*sides[:2], row),
        in_specs=[VMEM] * 4,
        out_specs=[VMEM] * 3,
        scratch_shapes=rows_scratch,
        name="other_sides",
    )(blocks, v, source, diagonal)
    halo = exchange(xa, xb, ya, yb)
    inner_sweep = call(
        inner_sweep_kernel, out_shape=field, in_specs=[VMEM] * 4, out_specs=VMEM, name="inner_sweep"
    )
    inner = inner_sweep(blocks, v, source, diagonal)
    relaxed, *second = call(
        outer_sweep_kernel,
        out_shape=(field, kept(nvar * ny + 16, nz), kept(nvar * ny + 16, nz)),
        in_specs=[VMEM] * 7,
        out_specs=[VMEM] * 3,
        name="outer_sweep",
    )(blocks, near_core(inner), diagonal, *halo)
    rows = halo[2], halo[3], near_core(ya), near_core(yb)

    halo = exchange(*second)
    inner = inner_sweep(blocks, near_core(relaxed), source, diagonal)
    smoothed, xa, xb, ya, yb, gradient = call(
        last_sweep_kernel,
        out_shape=(field, *sides, kept(NDES // 128, 128)),
        in_specs=[VMEM] * 13,
        out_specs=[VMEM] * 6,
        scratch_shapes=[
            pltpu.VMEM((nx * ny, nz), jnp.float32),
            pltpu.VMEM((nvar, nx, nz), jnp.float32),
            pltpu.VMEM((nvar, nx, nz), jnp.float32),
        ],
        name="last_sweep",
    )(
        blocks, near_core(inner), diagonal, *halo, *rows,
        sensitivity, mask, near_core(patch_band_slot), basis,
    )

    parts = lax.all_to_all(gradient, SPREAD, 0, 0, tiled=True)
    total = jnp.sum(parts, axis=0, keepdims=True)
    total = total + lax.ppermute(total, RING, [(i, i ^ 1) for i in range(8)])
    halo = exchange(xa, xb, ya, yb)
    total = total + lax.ppermute(total, RING, [(i, (((i + 1) ^ 1) - 1) % 8) for i in range(8)])
    across = [(0, 3), (3, 0), (1, 6), (6, 1), (2, 5), (5, 2), (4, 7), (7, 4)]
    other = lax.ppermute(total, RING, across)

    inner, smoothed = call(
        inner_residual_kernel,
        out_shape=(field, pltpu.HBM((nvar, nx, ny, nz), jnp.float32)),
        in_specs=[VMEM] * 4,
        out_specs=[VMEM, HBM],
        scratch_shapes=[pltpu.SemaphoreType.DMA],
        name="inner_residual",
    )(blocks, near_core(smoothed), source, diagonal)
    residual = call(
        outer_residual_kernel,
        out_shape=f32(nvar, nx, ny, nz),
        in_specs=[VMEM] * 6,
        out_specs=VMEM,
        name="outer_residual",
    )(blocks, near_core(inner), *halo)
    piece = NDES // 128
    start = lax.axis_index("yz_1") * piece
    design_gradient = lax.dynamic_slice(total + other, (0, start), (1, piece))
    return smoothed[None], residual[None], design_gradient.reshape(-1)


def solution(mesh):
    torus = Mesh(
        mesh.devices.reshape(mesh.shape["cond"], 4, 2, 4, 4),
        ("cond", "gx_0", "gx_1", "yz_0", "yz_1"),
    )
    in_specs = (
        P("cond", None, GX, YZ, None),
        P("cond", None, GX, YZ, None),
        P(GX, YZ, None),
        P("cond", None, None, None),
        P("cond", None, GX, YZ, None),
        P(GX, YZ, None),
        P(GX, YZ),
        P(),
        P(),
    )
    out_specs = (P("cond", None, GX, YZ, None), P("cond", None, GX, YZ, None), P(GX + YZ))
    return jax.shard_map(step, mesh=torus, in_specs=in_specs, out_specs=out_specs, check_vma=False)
```

```python
import jax
import jax.numpy as jnp
from jax import lax
from jax.experimental import pallas as pl
from jax.experimental.pallas import tpu as pltpu
from jax.sharding import Mesh
from jax.sharding import PartitionSpec as P


NDES = 4096
GX = ("gx_0", "gx_1")
YZ = ("yz_0", "yz_1")
RING = ("cond", "yz_1")
SPREAD = ("gx_0", "gx_1", "yz_0")
RELAXATION = 0.8
HIGHEST = lax.Precision.HIGHEST

VMEM = pl.BlockSpec(memory_space=pltpu.VMEM)
HBM = pl.BlockSpec(memory_space=pltpu.HBM)
SMEM = pl.BlockSpec(memory_space=pltpu.SMEM)


def f32(*shape):
    return jax.ShapeDtypeStruct(shape, jnp.float32)


def kept(*shape):
    return pltpu.VMEM(shape, jnp.float32)


def far_from_core(x):
    return pltpu.with_memory_space_constraint(x, pltpu.HBM)


def near_core(x):
    return pltpu.with_memory_space_constraint(x, pltpu.VMEM)


def call(kernel, **options):
    params = pltpu.CompilerParams(vmem_limit_bytes=8 * 2**20)
    return pl.pallas_call(kernel, compiler_params=params, **options)


def position():
    gx = lax.axis_index("gx_0") * 2 + lax.axis_index("gx_1")
    yz = lax.axis_index("yz_0") * 4 + lax.axis_index("yz_1")
    return gx, yz


def write_sides(read, nvar, nx, ny, xa_ref, xb_ref, ya_ref, yb_ref):
    gx, yz = position()
    gx_even, yz_even = lax.rem(gx, 2) == 0, lax.rem(yz, 2) == 0
    for k in range(nvar):
        low, high = read(k, 0), read(k, nx - 1)
        xa_ref[k] = jnp.where(gx_even, high, low)
        xb_ref[k] = jnp.where(gx_even, low, high)
        for x in range(nx):
            slab = read(k, x)
            first, last = slab[0:1], slab[ny - 1 : ny]
            ya_ref[k, x : x + 1, :] = jnp.where(yz_even, last, first)
            yb_ref[k, x : x + 1, :] = jnp.where(yz_even, first, last)


def coefficient(table_ref, d, e, k, nvar, shape):
    tile = table_ref[pl.ds((d * nvar + e) * nvar + k, 8, stride=0), :]
    rows = jnp.concatenate([tile] * (shape[0] // 8), axis=0)
    return jnp.concatenate([rows] * (shape[1] // 128), axis=1)


def load_kernel(
    blocks_hbm, weights_hbm, v_hbm, source_hbm, diagonal_hbm,
    v_ref, source_ref, diagonal_ref, table_ref, yb_ref,
    blocks_ref, weights_ref, next_ref, wanted_ref, sems,
):
    pairs = (
        (blocks_hbm, blocks_ref),
        (weights_hbm, weights_ref),
        (v_hbm, v_ref),
        (source_hbm, source_ref),
        (diagonal_hbm, diagonal_ref),
    )
    copies = [pltpu.make_async_copy(a, b, sems.at[i]) for i, (a, b) in enumerate(pairs)]
    for copy in copies:
        copy.start()
    nvar, _, _, _ = v_ref.shape
    for copy in copies[:2]:
        copy.wait()
    for d in range(6):
        for e in range(nvar):
            for k in range(nvar):
                row = (d * nvar + e) * nvar + k
                table_ref[row : row + 1, :] = jnp.full((1, 128), blocks_ref[e, k, 0, d])
    mine = jnp.where(lax.axis_index("cond") == 0, weights_ref[0], weights_ref[1])
    total = weights_ref[0].astype(jnp.float32) + weights_ref[1].astype(jnp.float32)
    one = jnp.ones((1, 128), jnp.float32)
    last = 6 * nvar * nvar
    table_ref[last : last + 1, :] = (one * mine.astype(jnp.float32)) / (one * total)
    for copy in copies[2:]:
        copy.wait()
    even = lax.rem(position()[1], 2) == 0
    relax_edge(table_ref, v_ref, source_ref, diagonal_ref, even, yb_ref, next_ref, wanted_ref)


def other_sides_kernel(
    table_ref, v_ref, source_ref, diagonal_ref, xa_ref, xb_ref, ya_ref, next_ref, wanted_ref
):
    nvar, nx, _, _ = v_ref.shape
    gx, yz = position()
    gx_even, yz_even = lax.rem(gx, 2) == 0, lax.rem(yz, 2) == 0
    for k in range(nvar):
        low, high = v_ref[k, 0], v_ref[k, nx - 1]
        xa_ref[k] = jnp.where(gx_even, high, low)
        xb_ref[k] = jnp.where(gx_even, low, high)
    relax_edge(table_ref, v_ref, source_ref, diagonal_ref, ~yz_even, ya_ref, next_ref, wanted_ref)


def relax_edge(table_ref, v_ref, source_ref, diagonal_ref, is_low, out_ref, next_ref, wanted_ref):
    nvar, nx, ny, nz = v_ref.shape
    for x in range(nx):
        here = slice(x, x + 1)
        out_ref[2 * nvar, here, :] = jnp.where(is_low, diagonal_ref[x, 0:1], diagonal_ref[x, ny - 1 : ny])
        for k in range(nvar):
            out_ref[k, here, :] = jnp.where(is_low, v_ref[k, x, 0:1], v_ref[k, x, ny - 1 : ny])
            next_ref[k, here, :] = jnp.where(is_low, v_ref[k, x, 1:2], v_ref[k, x, ny - 2 : ny - 1])
            wanted_ref[k, here, :] = jnp.where(is_low, source_ref[k, x, 0:1], source_ref[k, x, ny - 1 : ny])
    row = lax.broadcasted_iota(jnp.int32, (nx, nz), 0)
    lane = lax.broadcasted_iota(jnp.int32, (nx, nz), 1)
    sums = [0.0] * nvar
    for e in range(nvar):
        edge = out_ref[e]
        shifted = {
            0: jnp.where(row == nx - 1, 0.0, pltpu.roll(edge, nx - 1, 0)),
            1: jnp.where(row == 0, 0.0, pltpu.roll(edge, 1, 0)),
            4: jnp.where(lane == nz - 1, 0.0, pltpu.roll(edge, nz - 1, 1)),
            5: jnp.where(lane == 0, 0.0, pltpu.roll(edge, 1, 1)),
        }
        inward = next_ref[e]
        for k in range(nvar):
            for d, values in shifted.items():
                sums[k] = sums[k] + coefficient(table_ref, d, e, k, nvar, values.shape) * values
            both = [coefficient(table_ref, d, e, k, nvar, inward.shape) for d in (2, 3)]
            sums[k] = sums[k] + jnp.where(is_low, both[0], both[1]) * inward
    diagonal = out_ref[2 * nvar]
    scale = RELAXATION / diagonal
    for k in range(nvar):
        edge = out_ref[k]
        out_ref[nvar + k] = edge + scale * (wanted_ref[k] - diagonal * edge + sums[k])
    out_ref[2 * nvar] = scale


def neighbour_sums(v_ref, blocks_ref, x):
    nvar, nx, ny, nz = v_ref.shape
    row = lax.broadcasted_iota(jnp.int32, (ny, nz), 0)
    lane = lax.broadcasted_iota(jnp.int32, (ny, nz), 1)
    sums = [None] * nvar
    for e in range(nvar):
        centre = v_ref[e, x]
        shifted = {}
        if x + 1 < nx:
            shifted[0] = v_ref[e, x + 1]
        if x > 0:
            shifted[1] = v_ref[e, x - 1]
        shifted[2] = jnp.where(row == ny - 1, 0.0, pltpu.roll(centre, ny - 1, 0))
        shifted[3] = jnp.where(row == 0, 0.0, pltpu.roll(centre, 1, 0))
        shifted[4] = jnp.where(lane == nz - 1, 0.0, pltpu.roll(centre, nz - 1, 1))
        shifted[5] = jnp.where(lane == 0, 0.0, pltpu.roll(centre, 1, 1))
        for d, values in shifted.items():
            for k in range(nvar):
                term = coefficient(blocks_ref, d, e, k, nvar, values.shape) * values
                sums[k] = term if sums[k] is None else sums[k] + term
    return sums


def inner_sweep_kernel(blocks_ref, v_ref, source_ref, diagonal_ref, out_ref):
    nvar, nx, _, _ = v_ref.shape
    for x in range(nx):
        sums = neighbour_sums(v_ref, blocks_ref, x)
        diagonal = diagonal_ref[x]
        scale = RELAXATION / diagonal
        for k in range(nvar):
            value = v_ref[k, x]
            out_ref[k, x] = value + scale * (source_ref[k, x] - diagonal * value + sums[k])


def inner_residual_kernel(blocks_ref, v_ref, source_ref, diagonal_ref, out_ref, v_hbm, sem):
    copy = pltpu.make_async_copy(v_ref, v_hbm, sem)
    copy.start()
    nvar, nx, _, _ = v_ref.shape
    for x in range(nx):
        sums = neighbour_sums(v_ref, blocks_ref, x)
        diagonal = diagonal_ref[x]
        for k in range(nvar):
            out_ref[k, x] = source_ref[k, x] - diagonal * v_ref[k, x] + sums[k]
    copy.wait()


def add_halo(blocks_ref, inner_ref, diagonal_ref, xa, xb, ya, yb, out_ref):
    nvar, nx, ny, nz = inner_ref.shape
    gx, yz = position()
    gx_even, yz_even = lax.rem(gx, 2) == 0, lax.rem(yz, 2) == 0
    has_low_x, has_high_x = gx > 0, gx < 7
    has_low_y, has_high_y = yz > 0, yz < 15

    def halo_sums(direction, pick):
        sums = [None] * nvar
        for e in range(nvar):
            values = pick(e)
            for k in range(nvar):
                term = coefficient(blocks_ref, direction, e, k, nvar, values.shape) * values
                sums[k] = term if sums[k] is None else sums[k] + term
        return sums

    def picker(even, a, b, exists):
        return lambda e: jnp.where(exists, jnp.where(even, a(e), b(e)), 0.0)

    high_y = halo_sums(2, picker(yz_even, ya, yb, has_high_y))
    low_y = halo_sums(3, picker(yz_even, yb, ya, has_low_y))
    row = lax.broadcasted_iota(jnp.int32, (8, nz), 0)
    for x in range(nx):
        if x == 0:
            at_x = halo_sums(1, picker(gx_even, xb, xa, has_low_x))
        elif x == nx - 1:
            at_x = halo_sums(0, picker(gx_even, xa, xb, has_high_x))
        else:
            at_x = None
        for start in range(0, ny, 8):
            rows = slice(start, start + 8)
            scale = None if diagonal_ref is None else RELAXATION / diagonal_ref[x, rows]
            for k in range(nvar):
                more = None
                if start == 0:
                    more = jnp.where(row == 0, low_y[k][x : x + 1], 0.0)
                if start == ny - 8:
                    last = jnp.where(row == 7, high_y[k][x : x + 1], 0.0)
                    more = last if more is None else more + last
                if at_x is not None:
                    more = at_x[k][rows] if more is None else more + at_x[k][rows]
                value = inner_ref[k, x, rows]
                if more is not None:
                    value = value + (more if scale is None else scale * more)
                out_ref[k, x, rows] = value


def reader(ref):
    return lambda e: ref[e]


def outer_sweep_kernel(
    blocks_ref, inner_ref, diagonal_ref, xa_ref, xb_ref, ya_ref, yb_ref, out_ref, next_xa_ref, next_xb_ref,
):
    nvar, nx, ny, nz = inner_ref.shape
    halo = [reader(ref) for ref in (xa_ref, xb_ref, ya_ref, yb_ref)]
    add_halo(blocks_ref, inner_ref, diagonal_ref, *halo, out_ref)
    gx_even = lax.rem(position()[0], 2) == 0
    top = nvar * ny
    next_xa_ref[top:, :] = jnp.zeros((next_xa_ref.shape[0] - top, nz), jnp.float32)
    next_xb_ref[top:, :] = jnp.zeros((next_xb_ref.shape[0] - top, nz), jnp.float32)
    for k in range(nvar):
        low, high = out_ref[k, 0], out_ref[k, nx - 1]
        next_xa_ref[k * ny : (k + 1) * ny, :] = jnp.where(gx_even, high, low)
        next_xb_ref[k * ny : (k + 1) * ny, :] = jnp.where(gx_even, low, high)
        for start, ref in ((top, ya_ref), (top + nvar, yb_ref)):
            low, high = ref[k, 0:1], ref[k, nx - 1 : nx]
            next_xa_ref[start + k : start + k + 1, :] = jnp.where(gx_even, high, low)
            next_xb_ref[start + k : start + k + 1, :] = jnp.where(gx_even, low, high)


def complete_row(blocks_ref, xa_ref, xb_ref, top, is_low, far_ref, edge_ref, out_ref):
    nvar, nx, nz = out_ref.shape
    gx = position()[0]
    gx_even = lax.rem(gx, 2) == 0
    row = lax.broadcasted_iota(jnp.int32, (nx, nz), 0)
    at_low, at_high = (row == 0) & (gx > 0), (row == nx - 1) & (gx < 7)
    sums = [0.0] * nvar
    for e in range(nvar):
        edge = edge_ref[e]
        a, b = xa_ref[top + e : top + e + 1, :], xb_ref[top + e : top + e + 1, :]
        low = jnp.where(at_low, jnp.where(gx_even, b, a), 0.0)
        high = jnp.where(at_high, jnp.where(gx_even, a, b), 0.0)
        for k in range(nvar):
            both = [coefficient(blocks_ref, d, e, k, nvar, edge.shape) for d in (2, 3)]
            sums[k] = sums[k] + jnp.where(is_low, both[0], both[1]) * edge
            sums[k] = sums[k] + coefficient(blocks_ref, 1, e, k, nvar, edge.shape) * low
            sums[k] = sums[k] + coefficient(blocks_ref, 0, e, k, nvar, edge.shape) * high
    for k in range(nvar):
        out_ref[k] = far_ref[nvar + k] + far_ref[2 * nvar] * sums[k]


def select_kernel(slot_ref, onehot_ref):
    nx, ny = slot_ref.shape
    slots, patches = onehot_ref.shape
    pairs = slots // 2
    wanted = lax.broadcasted_iota(jnp.int32, (slots, patches), 0)
    wanted = jnp.where(wanted < pairs, 2 * wanted, 2 * (wanted - pairs) + 1)
    lane = lax.broadcasted_iota(jnp.int32, (ny, patches), 1)
    repeat = lax.rem(lane, ny) == lax.broadcasted_iota(jnp.int32, (ny, patches), 0)
    spread = jnp.dot(
        slot_ref[...].astype(jnp.float32), repeat.astype(jnp.float32), preferred_element_type=jnp.float32
    )
    lane = lax.broadcasted_iota(jnp.int32, (nx, patches), 1)
    own = lax.div(lane, ny) == lax.broadcasted_iota(jnp.int32, (nx, patches), 0)
    spread = jnp.sum(jnp.where(own, spread, 0.0), axis=0, keepdims=True)
    onehot_ref[...] = (wanted.astype(jnp.float32) == spread).astype(jnp.float32)


def last_sweep_kernel(
    blocks_ref, inner_ref, diagonal_ref, xa_ref, xb_ref, ya_ref, yb_ref, sent_ya_ref, sent_yb_ref,
    sensitivity_ref, mask_ref, onehot_ref, basis_ref,
    out_ref, next_xa_ref, next_xb_ref, next_ya_ref, next_yb_ref, gradient_ref, surface_ref, row_a_ref, row_b_ref,
):
    nvar, nx, ny, _ = inner_ref.shape
    even, top = lax.rem(position()[1], 2) == 0, nvar * ny
    complete_row(blocks_ref, xa_ref, xb_ref, top, ~even, ya_ref, sent_ya_ref, row_a_ref)
    complete_row(blocks_ref, xa_ref, xb_ref, top + nvar, even, yb_ref, sent_yb_ref, row_b_ref)
    add_halo(
        blocks_ref, inner_ref, diagonal_ref,
        lambda e: xa_ref[e * ny : (e + 1) * ny, :],
        lambda e: xb_ref[e * ny : (e + 1) * ny, :],
        reader(row_a_ref), reader(row_b_ref), out_ref,
    )
    write_sides(
        lambda k, x: out_ref[k, x], nvar, nx, ny, next_xa_ref, next_xb_ref, next_ya_ref, next_yb_ref
    )
    nvar, nx, ny, _ = inner_ref.shape
    for x in range(nx):
        total = out_ref[0, x] * sensitivity_ref[0, x].astype(jnp.float32)
        for k in range(1, nvar):
            total = total + out_ref[k, x] * sensitivity_ref[k, x].astype(jnp.float32)
        surface_ref[x * ny : (x + 1) * ny, :] = mask_ref[x].astype(jnp.float32) * total
    projected = jnp.dot(
        surface_ref[...], basis_ref[...], precision=HIGHEST, preferred_element_type=jnp.float32
    )
    _, band = projected.shape
    half = band // 2
    pairs = NDES // band
    onehot = onehot_ref[...].astype(jnp.bfloat16)
    by_slot, rest = None, projected
    for _ in range(3):
        part = rest.astype(jnp.bfloat16)
        rest = rest - part.astype(jnp.float32)
        term = jnp.dot(onehot, part, preferred_element_type=jnp.float32)
        by_slot = term if by_slot is None else by_slot + term
    even, odd = by_slot[:pairs], pltpu.roll(by_slot[pairs:], half, 1)
    row = lax.broadcasted_iota(jnp.int32, (pairs, band), 0)
    lane = lax.broadcasted_iota(jnp.int32, (pairs, band), 1)
    before = jnp.where(row == 0, 0.0, pltpu.roll(odd, 1, 0))
    gradient = even + jnp.where(lane < half, before, odd)
    share = blocks_ref[pl.ds(6 * nvar * nvar, 8, stride=0), :]
    gradient_ref[...] = gradient * jnp.concatenate([share] * (pairs // 8), axis=0)


def outer_residual_kernel(blocks_ref, inner_ref, xa_ref, xb_ref, ya_ref, yb_ref, out_ref):
    halo = [reader(ref) for ref in (xa_ref, xb_ref, ya_ref, yb_ref)]
    add_halo(blocks_ref, inner_ref, None, *halo, out_ref)


def swap_a(n):
    return [(i, i ^ 1) for i in range(n)]


def swap_b(n):
    return [(i, (((i + 1) ^ 1) - 1) % n) for i in range(n)]


def exchange(xa, xb, ya=None, yb=None):
    far = [] if yb is None else [lax.ppermute(yb, YZ, swap_b(16))]
    near = [] if ya is None else [lax.ppermute(ya, YZ, swap_a(16))]
    chip = lax.ppermute(xb, GX, swap_b(8))
    core = lax.ppermute(xa, GX, swap_a(8))
    return [near_core(x) for x in (core, chip, *near, *far)]


def step(
    adjoint,
    objective_gradient,
    diagonal,
    flux_blocks,
    flux_sensitivity,
    surface_mask,
    patch_band_slot,
    design_basis,
    condition_weights,
):
    sensitivity, mask = near_core(flux_sensitivity[0]), near_core(surface_mask)
    basis = near_core(design_basis)
    _, nvar, nx, ny, nz = adjoint.shape
    field = kept(nvar, nx, ny, nz)
    sides = (kept(nvar, ny, nz), kept(nvar, ny, nz), kept(nvar, nx, nz), kept(nvar, nx, nz))

    arrays = (flux_blocks.transpose(2, 3, 0, 1), condition_weights, adjoint[0], objective_gradient[0], diagonal)
    row = kept(2 * nvar + 1, nx, nz)
    rows_scratch = [pltpu.VMEM((nvar, nx, nz), jnp.float32)] * 2
    v, source, diagonal, blocks, yb = call(
        load_kernel,
        out_shape=(field, field, kept(nx, ny, nz), kept(6 * nvar * nvar + 1, 128), row),
        in_specs=[HBM] * 5,
        out_specs=[VMEM] * 5,
        scratch_shapes=[
            pltpu.SMEM((nvar, nvar, 1, 6), jnp.float32),
            pltpu.SMEM(condition_weights.shape, jnp.int32),
            *rows_scratch,
            pltpu.SemaphoreType.DMA((5,)),
        ],
        name="load",
    )(*(far_from_core(x) for x in arrays))
    v, source, diagonal, blocks = (near_core(x) for x in (v, source, diagonal, blocks))
    xa, xb, ya = call(
        other_sides_kernel,
        out_shape=(*sides[:2], row),
        in_specs=[VMEM] * 4,
        out_specs=[VMEM] * 3,
        scratch_shapes=rows_scratch,
        name="other_sides",
    )(blocks, v, source, diagonal)
    halo = exchange(xa, xb, ya, yb)
    inner_sweep = call(
        inner_sweep_kernel, out_shape=field, in_specs=[VMEM] * 4, out_specs=VMEM, name="inner_sweep"
    )
    inner = inner_sweep(blocks, v, source, diagonal)
    relaxed, *second = call(
        outer_sweep_kernel,
        out_shape=(field, kept(nvar * ny + 16, nz), kept(nvar * ny + 16, nz)),
        in_specs=[VMEM] * 7,
        out_specs=[VMEM] * 3,
        name="outer_sweep",
    )(blocks, near_core(inner), diagonal, *halo)
    rows = halo[2], halo[3], near_core(ya), near_core(yb)

    halo = exchange(*second)
    inner = inner_sweep(blocks, near_core(relaxed), source, diagonal)
    onehot = call(
        select_kernel,
        out_shape=kept(2 * NDES // 128, nx * ny),
        in_specs=[VMEM],
        out_specs=VMEM,
        name="select",
    )(near_core(patch_band_slot))
    smoothed, xa, xb, ya, yb, gradient = call(
        last_sweep_kernel,
        out_shape=(field, *sides, kept(NDES // 128, 128)),
        in_specs=[VMEM] * 13,
        out_specs=[VMEM] * 6,
        scratch_shapes=[
            pltpu.VMEM((nx * ny, nz), jnp.float32),
            pltpu.VMEM((nvar, nx, nz), jnp.float32),
            pltpu.VMEM((nvar, nx, nz), jnp.float32),
        ],
        name="last_sweep",
    )(
        blocks, near_core(inner), diagonal, *halo, *rows,
        sensitivity, mask, near_core(onehot), basis,
    )

    parts = lax.all_to_all(gradient, SPREAD, 0, 0, tiled=True)
    total = jnp.sum(parts, axis=0, keepdims=True)
    total = total + lax.ppermute(total, RING, [(i, i ^ 1) for i in range(8)])
    halo = exchange(xa, xb, ya, yb)
    total = total + lax.ppermute(total, RING, [(i, (((i + 1) ^ 1) - 1) % 8) for i in range(8)])
    across = [(0, 3), (3, 0), (1, 6), (6, 1), (2, 5), (5, 2), (4, 7), (7, 4)]
    other = lax.ppermute(total, RING, across)

    inner, smoothed = call(
        inner_residual_kernel,
        out_shape=(field, pltpu.HBM((nvar, nx, ny, nz), jnp.float32)),
        in_specs=[VMEM] * 4,
        out_specs=[VMEM, HBM],
        scratch_shapes=[pltpu.SemaphoreType.DMA],
        name="inner_residual",
    )(blocks, near_core(smoothed), source, diagonal)
    residual = call(
        outer_residual_kernel,
        out_shape=f32(nvar, nx, ny, nz),
        in_specs=[VMEM] * 6,
        out_specs=VMEM,
        name="outer_residual",
    )(blocks, near_core(inner), *halo)
    piece = NDES // 128
    start = lax.axis_index("yz_1") * piece
    design_gradient = lax.dynamic_slice(total + other, (0, start), (1, piece))
    return smoothed[None], residual[None], design_gradient.reshape(-1)


def solution(mesh):
    torus = Mesh(
        mesh.devices.reshape(mesh.shape["cond"], 4, 2, 4, 4),
        ("cond", "gx_0", "gx_1", "yz_0", "yz_1"),
    )
    in_specs = (
        P("cond", None, GX, YZ, None),
        P("cond", None, GX, YZ, None),
        P(GX, YZ, None),
        P("cond", None, None, None),
        P("cond", None, GX, YZ, None),
        P(GX, YZ, None),
        P(GX, YZ),
        P(),
        P(),
    )
    out_specs = (P("cond", None, GX, YZ, None), P("cond", None, GX, YZ, None), P(GX + YZ))
    return jax.shard_map(step, mesh=torus, in_specs=in_specs, out_specs=out_specs, check_vma=False)
```
